32 devices in a mesh: dp: 16 (over z, y, x), mp: 2 (over core).
Axes of the slice: x: 2, y: 2, z: 4, core: 2. Of those that a mesh axis runs over, the one named last changes fastest.
Arguments:
- points: bfloat16 [16384, 1024], P(('dp', 'mp')), may hold values from -6 to 6
- centroids: bfloat16 [4096, 1024], P('mp'), may hold values from -6 to 6
- assign: int32 [16384], P(('dp', 'mp')), may hold values from 0 to 4095
- keep_mask: int32 [16384], P(('dp', 'mp')), may hold values 0 or 1
Outputs:
- new_centroids: float32 [4096, 1024], P('mp')
- row_cost: float32 [16384], P(('dp', 'mp'))
The draws below stay inside these ranges and needn't reach their ends.
All inputs are finite; a program needn't handle non-finite values. No bound on the sum of `keep_mask` on one device may be relied on, other than what follows from the above.
Results may differ from the reference program's by a relative error of at most 0.0008.
Values may be sent and summed in bfloat16 or wider, within the bound.
A program may use at most 128 MiB of HBM per device.

```python
import math
import jax
import jax.numpy as jnp
import numpy as np
from jax import lax

D = 1024
K = 4096
ROWS = 16384


def place_ends(values, stream_key, smallest, high):
    longest = values.shape.index(max(values.shape))
    spots = []
    for shift in (0, 1):
        where = [jax.random.randint(jax.random.fold_in(stream_key, axis), (), 0, length) for axis, length in enumerate(values.shape)]
        where[longest] = (where[longest] + shift) % values.shape[longest]
        spots.append(tuple(where))
    return values.at[spots[0]].set(smallest).at[spots[1]].set(high)


def block_scale(own_key, dims, shards, smallest, high):
    level = 1.0
    for axis_at, shards_of in shards:
        draws = jax.random.uniform(jax.random.fold_in(jax.random.fold_in(own_key, 6), axis_at), (shards_of,), jnp.float32, smallest / len(shards), high / len(shards))
        level = level * jnp.repeat(jnp.exp(draws), dims[axis_at] // shards_of).reshape((-1,) + (1,) * (len(dims) - 1 - axis_at))
    return level


def cumulative_ranks(count, lean):
    portions = [(1 << 20) // math.isqrt(standing ** lean) + 1 for standing in range(1, count + 1)]
    width = 1 + sum(portions) // (1 << 30)
    return np.cumsum(np.array([max(1, weight // width) for weight in portions]))


def skewed_ids(own_key, extent, count, skew):
    grid = cumulative_ranks(count, skew)
    pick = jax.random.randint(jax.random.fold_in(own_key, 1), extent, 0, int(grid[count - 1]))
    standing = jnp.searchsorted(jnp.asarray(grid, jnp.int32), pick, side="right")
    return jax.random.permutation(jax.random.fold_in(own_key, 2), count)[standing].astype(jnp.int32)


def centred(own_key, shape, deviation, limit, cuts=(), kind=jnp.bfloat16):
    result = deviation * jax.random.normal(own_key, shape, jnp.float32)
    if cuts:
        result = result * block_scale(own_key, shape, cuts, -0.22, 0.18)
    return jnp.clip(result, -limit, limit).astype(kind)


def setup_inputs(seed: int = 0) -> dict:
    seeds = jax.random.split(jax.random.key(seed), 5)
    points = centred(seeds[0], (ROWS, D), 1.0, 6.0, ((0, 32),))
    centroids = centred(seeds[1], (K, D), 1.0, 6.0, ((0, 2),))
    assign = place_ends(skewed_ids(seeds[2], (ROWS,), K, 2), jax.random.fold_in(seeds[2], 3), 0, K - 1).astype(jnp.int32)
    keep_mask = place_ends((jax.random.randint(seeds[3], (ROWS,), 0, 4) < 3).astype(jnp.int32), jax.random.fold_in(seeds[3], 1), 0, 1)
    return dict(points=points, centroids=centroids, assign=assign, keep_mask=keep_mask)


def reference(points, centroids, assign, keep_mask):
    cent_f = centroids.astype(jnp.float32)
    cent_sq = jnp.sum(cent_f * cent_f, axis=1)
    block = math.gcd(ROWS, 1024)
    blocks = points.reshape(ROWS // block, block, D)

    def cost_block(group_rows):
        point_f = group_rows.astype(jnp.float32)
        point_sq = jnp.sum(point_f * point_f, axis=1)
        inner = jnp.dot(group_rows, centroids.T, preferred_element_type=jnp.float32)
        dist = point_sq[:, None] - 2.0 * inner + cent_sq[None, :]
        return jnp.min(dist, axis=1) / D

    row_cost = lax.map(cost_block, blocks).reshape(ROWS)
    weights = keep_mask.astype(jnp.float32)
    sums = jax.ops.segment_sum(points.astype(jnp.float32) * weights[:, None], assign, num_segments=K)
    counts = jax.ops.segment_sum(weights, assign, num_segments=K)
    fresh = sums / jnp.maximum(counts, 1.0)[:, None]
    new_centroids = jnp.where(counts[:, None] > 0.5, fresh, cent_f)
    return new_centroids, row_cost
```

```python
import functools

import jax
import jax.numpy as jnp
from jax import lax
from jax.experimental import pallas as pl
from jax.experimental.pallas import tpu as pltpu
from jax.sharding import Mesh
from jax.sharding import PartitionSpec as P

STEPS = 32000.0
TINY = 2.0**-100
BIAS = 128
WORD = 24
PLANE = 4
LANES = 128
CTILE = 256
MESH = pl.DeviceIdType.MESH


def remote(src, dst, send, recv, device):
    return pltpu.make_async_remote_copy(
        src_ref=src, dst_ref=dst, send_sem=send, recv_sem=recv, device_id=device, device_id_type=MESH
    )


def power_of(top):
    return jnp.ceil(jnp.log2(jnp.maximum(top, TINY)))


def quantize(v, power):
    return jnp.floor(v * (jnp.exp2(-power) * STEPS) + 0.5).astype(jnp.int32)


def embed(code, word):
    lane = lax.broadcasted_iota(jnp.int32, code.shape, 1)
    bit = lax.shift_right_logical(jnp.broadcast_to(word, code.shape), jnp.minimum(lane, 31)) & 1
    return (code & jnp.where(lane < WORD, -2, -1)) | bit


def pack(code):
    half = code.shape[0] // 2
    return (code[:half] << 16) | (code[half:] & 0xFFFF)


def unpack(packed):
    return jnp.concatenate([packed >> 16, (packed << 16) >> 16], axis=0)


def word_of(code):
    lane = lax.broadcasted_iota(jnp.int32, (1, LANES), 1)
    weight = jnp.where(lane < WORD, 1 << jnp.minimum(lane, WORD), 0).astype(jnp.float32)
    return jnp.sum((code & 1).astype(jnp.float32) * weight, axis=1, keepdims=True).astype(jnp.int32)


def scale_of(word):
    return jnp.exp2(((word & 255) - BIAS).astype(jnp.float32)) / STEPS


def encode(v, count=None):
    power = power_of(jnp.max(jnp.abs(v), axis=1, keepdims=True))
    word = power.astype(jnp.int32) + BIAS
    if count is not None:
        word = word + (count.astype(jnp.int32) << 8)
    return pack(embed(quantize(v, power), word))


def decode(packed):
    code = unpack(packed)
    word = word_of(code)
    return code.astype(jnp.float32) * scale_of(word), (word >> 8).astype(jnp.float32)


def update_kernel(
    z_n, pairs, p_hbm, c_hbm, assign_ref, keep_ref, out_ref, cost_ref,
    p2, cents, prior, idv, slot, hit, pn, acc, cnt, asend, arecv, zsend, zrecv, low, lowr,
    loc, ids_s, ids_r, mt_s, mt_r, ps, pr, fs, fr, as_, ar, zs, zr,
    grs, grr, gls, glr, xs, xr, ys, yr, ds_, dr, lo_s, lo_r,
):
    z, q, m = lax.axis_index("z"), lax.axis_index("q"), lax.axis_index("mp")
    nx = q + 1 - 2 * lax.rem(q, 2)
    ny = lax.rem(q + 2, PLANE)
    other = 1 - m
    rows, width = p_hbm.shape
    shard_rows = c_hbm.shape[0]
    block = prior.shape[0]
    both = 2 * rows
    kept = z_n * block
    side_w = width // 2
    part = side_w // pairs
    last = z_n - 1
    up, down = lax.rem(z + 1, z_n), lax.rem(z + last, z_n)
    own = z * PLANE + q
    near, far = (nx, ny), (ny, nx)

    load_p = pltpu.make_async_copy(p_hbm, p2.at[pl.ds(0, rows)], loc.at[0])
    load_prior = pltpu.make_async_copy(
        c_hbm.at[pl.ds(pl.multiple_of(own * block, block), block)], prior, loc.at[1]
    )
    load_c = pltpu.make_async_copy(c_hbm, cents, loc.at[2])
    load_p.start()
    idv[0] = jnp.where(keep_ref[...] > 0, assign_ref[...], -1)

    barrier = pltpu.get_barrier_semaphore()
    peers = [(z, q, other), (z, nx, m), (z, nx, other), (z, ny, m), (z, ny, other)]
    greet = peers + [(lax.rem(z + k, z_n), q, m) for k in range(1, z_n)]
    for peer in greet:
        pl.semaphore_signal(barrier, inc=1, device_id=peer, device_id_type=MESH)
    load_c.start()
    load_prior.start()
    pl.semaphore_wait(barrier, len(greet))

    def pts_copy(s, p):
        cols = pl.ds(s * side_w + p * part, part)
        return remote(
            p2.at[pl.ds(0, rows), cols], pn.at[s, p, pl.ds(0, rows)], ps.at[s, p], pr.at[s, p],
            (z, near[s], m),
        )

    def fwd_copy(s, p):
        return remote(
            pn.at[s, p, pl.ds(0, rows)], pn.at[s, p, pl.ds(rows, rows)], fs.at[s, p], fr.at[s, p],
            (z, q, other),
        )

    def a_copy(s, p):
        return remote(asend.at[s, p], arecv.at[s, p], as_.at[s, p], ar.at[s, p], (z, far[s], m))

    def z_copy(p, k):
        to = lax.rem(z + k, z_n)
        return remote(zsend.at[p, to], zrecv.at[p, k], zs.at[p, k], zr.at[p, k], (to, q, m))

    id_copies = [
        remote(idv.at[0], idv.at[k + 1], ids_s.at[k], ids_r.at[k], peer) for k, peer in enumerate(peers)
    ]
    mate_copy = remote(p2.at[pl.ds(0, rows)], p2.at[pl.ds(rows, rows)], mt_s, mt_r, (z, q, other))

    load_p.wait()
    for copy in id_copies:
        copy.start()
    for s in range(2):
        pts_copy(s, 0).start()
    mate_copy.start()
    for p in range(1, pairs - 1):
        for s in range(2):
            pts_copy(s, p).start()
    for copy in id_copies:
        copy.wait_recv()

    def slots_of(s, a, b):
        ids = jnp.concatenate([idv[a], idv[b]], axis=1) - m * shard_rows
        inside = (ids >= 0) & (ids < shard_rows)
        ids = jnp.where(inside, ids, 0)
        owner = lax.rem(lax.div(ids, block), PLANE)
        at = lax.div(ids, block * PLANE) * block + lax.rem(ids, block)
        found = jnp.where(owner == q, at, jnp.where(owner == far[s], at + kept, -1))
        return jnp.where(inside, found, -1)

    def fill_hits(s, group, first):
        slot[s] = slots_of(s, *((0, 1) if first else ((2, 3), (4, 5))[s]))

        def tile(t, carry):
            base = pl.multiple_of(t * LANES, LANES)
            row = lax.broadcasted_iota(jnp.int32, (LANES, both), 0) + base
            found = jnp.where(row == slot[s], 1.0, 0.0)
            hit[group, pl.ds(base, LANES), :] = found.astype(jnp.bfloat16)
            if s == 0:
                count = jnp.broadcast_to(jnp.sum(found, axis=1, keepdims=True), (LANES, LANES))
                at = pl.ds(base, LANES)
                cnt[at, :] = count if first else cnt[at, :] + count
            return carry

        lax.fori_loop(0, 2 * kept // LANES, tile, 0)

    def own_dots(s):
        def tile(t, carry):
            at = pl.ds(pl.multiple_of(t * kept, kept), kept)
            acc[s, at, :] = jnp.dot(
                hit[s, at, :], p2[:, s * side_w : (s + 1) * side_w], preferred_element_type=jnp.float32
            )
            return carry

        lax.fori_loop(0, 2, tile, 0)

    def near_dot(s, p, half):
        at, cols = pl.ds(half * kept, kept), pl.ds(p * part, part)
        acc[s, at, cols] += jnp.dot(hit[s, at, :], pn[s, p], preferred_element_type=jnp.float32)

    def rows_of(t):
        return pl.ds(pl.multiple_of(t * block, block), block)

    def half_rows_of(t):
        return pl.ds(pl.multiple_of(t * (block // 2), block // 2), block // 2)

    def step_b(p):
        for s in range(2):
            pts_copy(s, p).wait_recv()
            fwd_copy(s, p).start()
        for s in range(2):
            fwd_copy(s, p).wait_recv()
            near_dot(s, p, 1)

            def tile(t, carry, s=s):
                at = pl.ds(pl.multiple_of(kept + t * block, block), block)
                count = cnt[at, 0:1] if s == 0 and p == 0 else None
                asend[s, p, half_rows_of(t), :] = encode(acc[s, at, p * part : (p + 1) * part], count)
                return carry

            lax.fori_loop(0, z_n, tile, 0)
            a_copy(s, p).start()
        for s in range(2):
            near_dot(s, p, 0)

    def step_c(p):
        for s in range(2):
            a_copy(s, p).wait_recv()

            def tile(t, carry, s=s):
                at = rows_of(t)
                more, count = decode(arecv[s, p, half_rows_of(t), :])
                v = acc[s, at, p * part : (p + 1) * part] + more
                acc[s, at, p * part : (p + 1) * part] = v
                if s == 0 and p == 0:
                    total = cnt[at, 0:1] + count
                    cnt[at, :] = jnp.broadcast_to(total, (block, LANES))
                else:
                    total = None
                zsend[p, t, s * (block // 2) : (s + 1) * (block // 2), :] = encode(v, total)
                return carry

            lax.fori_loop(0, z_n, tile, 0)
        for k in range(1, z_n):
            z_copy(p, k).start()

    def xcopy(p, n, to_q):
        at = out_ref.at[p, n * PLANE + to_q]
        return remote(at, at, xs.at[p, n], xr.at[p, n], (z, nx, m))

    def ycopy(p, n, to_q):
        at = out_ref.at[p, n * PLANE + to_q]
        return remote(at, at, ys.at[p, n], yr.at[p, n], (z, ny, m))

    def dcopy(p, n, by_x):
        at = out_ref.at[p, n * PLANE + (nx if by_x else ny)]
        return remote(at, at, ds_.at[p, n], dr.at[p, n], (z, ny if by_x else nx, m))

    def gright(p, n):
        at = out_ref.at[p, n * PLANE + q]
        return remote(at, at, grs.at[p, n], grr.at[p, n], (up, q, m))

    def gleft(p, n):
        at = out_ref.at[p, n * PLANE + q]
        return remote(at, at, gls.at[p, n], glr.at[p, n], (down, q, m))

    def step_d(p):
        mine = rows_of(z)
        for k in range(1, z_n):
            z_copy(p, k).wait_recv()
        if p == 0:
            load_prior.wait()
        fresh = []
        for s in range(2):
            total = acc[s, mine, p * part : (p + 1) * part]
            count = cnt[mine, 0:1]
            for k in range(1, z_n):
                more, extra = decode(zrecv[p, k, s * (block // 2) : (s + 1) * (block // 2), :])
                total = total + more
                count = count + extra
            if p == 0 and s == 0:
                cnt[mine, :] = jnp.broadcast_to(count, (block, LANES))
            count = cnt[mine, 0:1]
            lo = s * side_w + p * part
            fallback = prior[:, lo : lo + part].astype(jnp.float32)
            fresh.append(jnp.where(count > 0.5, total / jnp.maximum(count, 1.0), fallback))
        top = jnp.max(jnp.maximum(jnp.abs(fresh[0]), jnp.abs(fresh[1])), axis=1, keepdims=True)
        power = power_of(top)
        word = power.astype(jnp.int32) + BIAS
        out_ref[p, own, : block // 2] = pack(embed(quantize(fresh[0], power), word))
        out_ref[p, own, block // 2 :] = pack(quantize(fresh[1], power))

        @pl.when(z < last)
        def _():
            gright(p, z).start()

        @pl.when(z > 0)
        def _():
            gleft(p, z).start()

        xcopy(p, z, q).start()
        ycopy(p, z, q).start()

    def relay(p, n, by_x):
        if by_x:
            xcopy(p, n, nx).wait_recv()
        else:
            ycopy(p, n, ny).wait_recv()
        dcopy(p, n, by_x).start()

    def settle(p, n, by_x):
        if by_x:
            ycopy(p, n, ny).wait_recv()
        else:
            xcopy(p, n, nx).wait_recv()
        dcopy(p, n, by_x).wait_recv()

    def each(p, k, action):
        if k == 0:
            action(p, z, p % 2 == 0)
            return

        @pl.when(z >= k)
        def _():
            action(p, z - k, (k + p) % 2 == 0)

        @pl.when(z + k <= last)
        def _():
            action(p, z + k, (k + p) % 2 == 1)

    def spread(p, k):
        @pl.when(z >= k)
        def _():
            gright(p, z - k).wait_recv()

            @pl.when(z < last)
            def _():
                gright(p, z - k).start()

            xcopy(p, z - k, q).start()
            ycopy(p, z - k, q).start()

        @pl.when(z + k <= last)
        def _():
            gleft(p, z + k).wait_recv()

            @pl.when(z > 0)
            def _():
                gleft(p, z + k).start()

            xcopy(p, z + k, q).start()
            ycopy(p, z + k, q).start()

    def lowest(i, n):
        if i == 0:
            load_c.wait()

        def tile(t, best):
            tile_ref = cents[pl.ds(pl.multiple_of(t * CTILE, CTILE), CTILE), :]
            wide = tile_ref.astype(jnp.float32)
            sq = jnp.sum(wide * wide, axis=1, keepdims=True)
            inner = lax.dot_general(
                tile_ref, p2[...], (((1,), (1,)), ((), ())), preferred_element_type=jnp.float32
            )
            return jnp.minimum(best, jnp.min(sq - 2.0 * inner, axis=0, keepdims=True))

        start = jnp.full((1, both), jnp.inf, jnp.float32) if i == 0 else low[...]
        low[...] = lax.fori_loop(i * n, (i + 1) * n, tile, start)

    low_copy = remote(low.at[:, pl.ds(rows, rows)], lowr, lo_s, lo_r, (z, q, other))

    def finish_cost():
        low_copy.wait_recv()
        wide = p2[pl.ds(0, rows), :].astype(jnp.float32)
        sq = jnp.sum(wide * wide, axis=1, keepdims=True)
        flat = jnp.broadcast_to(sq, (rows, LANES)).T[0:1, :]
        cost_ref[...] = (flat + jnp.minimum(low[:, :rows], lowr[...])) / width

    mate_copy.wait_recv()
    for s in range(2):
        fill_hits(s, s, True)
        own_dots(s)
    for s in range(2):
        fill_hits(s, s, False)

    tasks = [(i, step_b, (i,)) for i in range(pairs - 1)]
    tasks += [(2.5 + i, step_c, (i,)) for i in range(pairs)]
    tasks += [(2.7, lambda: [pts_copy(s, pairs - 1).start() for s in range(2)], ())]
    tasks[-1] = (0.5, tasks[-1][1], ())
    tasks += [(3.2, step_b, (pairs - 1,))]
    pieces = shard_rows // CTILE // 2
    for p in range(pairs):
        base = (4.8, 6, 8, 10)[p]
        tasks.append((base, step_d, (p,)))
        for k in range(1, z_n):
            tasks.append((base + 1.2 * k, spread, (p, k)))
        for k in range(z_n):
            tasks.append((base + 1.2 * k + 1.0, each, (p, k, relay)))
            tasks.append((100 + p + 0.01 * k, each, (p, k, settle)))
    for i in range(pieces):
        tasks.append((5.55 + i, lowest, (i, 2)))
    tasks.append((5.6 + pieces, low_copy.start, ()))
    tasks.append((8.7 + pieces, finish_cost, ()))
    for _, action, args in sorted(tasks, key=lambda task: task[0]):
        action(*args)

    for copy in id_copies + [mate_copy, low_copy]:
        copy.wait_send()
    for p in range(pairs):
        for s in range(2):
            pts_copy(s, p).wait_send()
            fwd_copy(s, p).wait_send()
            a_copy(s, p).wait_send()
        for t in range(z_n):
            if t > 0:
                z_copy(p, t).wait_send()

            @pl.when((z >= t) & (z < last))
            def _(p=p, t=t):
                gright(p, t).wait_send()

            @pl.when((z <= t) & (z > 0))
            def _(p=p, t=t):
                gleft(p, t).wait_send()

            xcopy(p, t, q).wait_send()
            ycopy(p, t, q).wait_send()
            dcopy(p, t, True).wait_send()


def decode_kernel(pairs, in_ref, out_ref):
    owners, block = in_ref.shape[1], in_ref.shape[2]
    half = block // 2
    side_w = out_ref.shape[1] // 2
    part = side_w // pairs
    for o in range(owners):
        at = slice(o * block, (o + 1) * block)
        for p in range(pairs):
            first = unpack(in_ref[p, o, :half])
            scale = scale_of(word_of(first))
            out_ref[at, p * part : (p + 1) * part] = first.astype(jnp.float32) * scale
            second = unpack(in_ref[p, o, half:])
            out_ref[at, side_w + p * part : side_w + (p + 1) * part] = second.astype(jnp.float32) * scale


def shards(points, centroids, assign, keep_mask):
    rows, width = points.shape
    shard_rows = centroids.shape[0]
    z_n = lax.axis_size("z")
    dp_n = z_n * PLANE
    block = shard_rows // dp_n
    kept = z_n * block
    part = LANES
    side_w = width // 2
    pairs = side_w // part
    vmem = pl.BlockSpec(memory_space=pltpu.VMEM)
    hbm = pl.BlockSpec(memory_space=pl.ANY)
    dma = pltpu.SemaphoreType.DMA
    by_pair = dma((2, pairs))
    by_z = dma((pairs, z_n))
    back, cost = pl.pallas_call(
        functools.partial(update_kernel, z_n, pairs),
        out_shape=(
            jax.ShapeDtypeStruct((pairs, dp_n, block, part), jnp.int32),
            jax.ShapeDtypeStruct((1, rows), jnp.float32),
        ),
        in_specs=[hbm, hbm, vmem, vmem],
        out_specs=(vmem, vmem),
        scratch_shapes=[
            pltpu.VMEM((2 * rows, width), points.dtype),
            pltpu.VMEM((shard_rows, width), centroids.dtype),
            pltpu.VMEM((block, width), centroids.dtype),
            pltpu.VMEM((6, 1, rows), jnp.int32),
            pltpu.VMEM((2, 1, 2 * rows), jnp.int32),
            pltpu.VMEM((2, 2 * kept, 2 * rows), jnp.bfloat16),
            pltpu.VMEM((2, pairs, 2 * rows, part), points.dtype),
            pltpu.VMEM((2, 2 * kept, side_w), jnp.float32),
            pltpu.VMEM((2 * kept, LANES), jnp.float32),
            pltpu.VMEM((2, pairs, kept // 2, part), jnp.int32),
            pltpu.VMEM((2, pairs, kept // 2, part), jnp.int32),
            pltpu.VMEM((pairs, z_n, block, part), jnp.int32),
            pltpu.VMEM((pairs, z_n, block, part), jnp.int32),
            pltpu.VMEM((1, 2 * rows), jnp.float32),
            pltpu.VMEM((1, rows), jnp.float32),
            dma((3,)), dma((5,)), dma((5,)), dma, dma,
            by_pair, by_pair, by_pair, by_pair, by_pair, by_pair,
            by_z, by_z, by_z, by_z, by_z, by_z, by_z, by_z, by_z, by_z, by_z, by_z,
            dma, dma,
        ],
        compiler_params=pltpu.CompilerParams(
            collective_id=0, has_side_effects=True, vmem_limit_bytes=40 * 1024 * 1024
        ),
        cost_estimate=pl.CostEstimate(
            flops=0, bytes_accessed=200 * 1024 * 1024, transcendentals=0
        ),
        name="update",
    )(points, centroids, assign.reshape(1, rows), keep_mask.reshape(1, rows))
    owners = max(1, min(dp_n, 512 // block))
    new_centroids = pl.pallas_call(
        functools.partial(decode_kernel, pairs),
        grid=(dp_n // owners,),
        in_specs=[pl.BlockSpec((pairs, owners, block, part), lambda i: (0, i, 0, 0))],
        out_specs=pl.BlockSpec((owners * block, width), lambda i: (i, 0)),
        out_shape=jax.ShapeDtypeStruct((shard_rows, width), jnp.float32),
        cost_estimate=pl.CostEstimate(
            flops=0, bytes_accessed=12 * 1024 * 1024, transcendentals=0
        ),
        name="decode",
    )(back)
    return new_centroids, cost.reshape(rows)


def solution(mesh):
    dp, mp = mesh.shape["dp"], mesh.shape["mp"]
    grid = Mesh(mesh.devices.reshape(dp // PLANE, PLANE, mp), ("z", "q", "mp"))
    rows = ("z", "q", "mp")
    in_specs = (P(rows, None), P("mp", None), P(rows), P(rows))
    out_specs = (P("mp", None), P(rows))
    return jax.shard_map(shards, mesh=grid, in_specs=in_specs, out_specs=out_specs, check_vma=False)
```

```python
import functools

import jax
import jax.numpy as jnp
from jax import lax
from jax.experimental import pallas as pl
from jax.experimental.pallas import tpu as pltpu
from jax.sharding import Mesh
from jax.sharding import PartitionSpec as P

STEPS = 32000.0
TINY = 2.0**-100
BIAS = 128
EXP = 8
WORD = 32
GROUP = 16
FINE = 8.0
FINE_BIAS = 1024
FINE_BITS = 12
PLANE = 4
LATE = 2
LANES = 128
CTILE = 256
MESH = pl.DeviceIdType.MESH


def remote(src, dst, send, recv, device):
    return pltpu.make_async_remote_copy(
        src_ref=src, dst_ref=dst, send_sem=send, recv_sem=recv, device_id=device, device_id_type=MESH
    )


def power_of(top):
    return jnp.ceil(jnp.log2(jnp.maximum(top, TINY)))


def quantize(v, power):
    return jnp.floor(v * (jnp.exp2(-power) * STEPS) + 0.5).astype(jnp.int32)


def embed(code, power, count=None):
    lane = lax.broadcasted_iota(jnp.int32, code.shape, 1)
    bit = lax.shift_right_logical(jnp.broadcast_to(power, code.shape), jnp.minimum(lane, 31)) & 1
    used = EXP
    if count is not None:
        at = jnp.clip(lane - EXP, 0, 31)
        bit = jnp.where(lane < EXP, bit, lax.shift_right_logical(jnp.broadcast_to(count, code.shape), at) & 1)
        used = WORD
    return (code & jnp.where(lane < used, -2, -1)) | bit


def pack(code):
    half = code.shape[0] // 2
    return (code[:half] << 16) | (code[half:] & 0xFFFF)


def unpack(packed):
    return jnp.concatenate([packed >> 16, (packed << 16) >> 16], axis=0)


def bits_word(code, lo, hi):
    lane = lax.broadcasted_iota(jnp.int32, (1, LANES), 1)
    weight = jnp.where((lane >= lo) & (lane < hi), 1 << jnp.clip(lane - lo, 0, hi - lo), 0)
    bits = (code[:, :LANES] & 1).astype(jnp.float32)
    return jnp.sum(bits * weight.astype(jnp.float32), axis=1, keepdims=True)


def scale_of(code):
    return jnp.exp2(bits_word(code, 0, EXP) - BIAS) * (1.0 / STEPS)


def count_of(code):
    return bits_word(code, EXP, WORD)


def encode(v, count=None):
    power = power_of(jnp.max(jnp.abs(v), axis=1, keepdims=True))
    if count is not None:
        count = count.astype(jnp.int32)
    return pack(embed(quantize(v, power), power.astype(jnp.int32) + BIAS, count))


def decode(packed):
    code = unpack(packed)
    return code.astype(jnp.float32) * scale_of(code)


def group_of(half):
    return min(GROUP, half)


def publish_code(v):
    half = v.shape[0] // 2
    size = group_of(half)
    lane = lax.broadcasted_iota(jnp.int32, (size, LANES), 1)
    out = []
    for g in range(half // size):
        hi, lo = v[g * size : (g + 1) * size], v[half + g * size : half + (g + 1) * size]
        top = jnp.max(jnp.maximum(jnp.abs(hi), jnp.abs(lo)), axis=0, keepdims=True)
        top = jnp.maximum(jnp.max(top, axis=1, keepdims=True), TINY)
        word = jnp.ceil(jnp.log2(top) * FINE)
        factor = jnp.exp2(word * (-1.0 / FINE)) * STEPS
        codes = [jnp.floor(part * factor + 0.5).astype(jnp.int32) for part in (hi, lo)]
        bit = lax.shift_right_logical(
            jnp.broadcast_to(word.astype(jnp.int32) + FINE_BIAS, (size, LANES)), jnp.minimum(lane, 31)
        ) & 1
        first = (codes[0] & jnp.where(lane < FINE_BITS, -2, -1)) | jnp.where(lane < FINE_BITS, bit, 0)
        out.append((first << 16) | (codes[1] & 0xFFFF))
    return jnp.concatenate(out, axis=0)


TUNED = {
    (4, 4, 8): (
        0, 10, 19, 23, 34, 1, 11, 16, 30, 33, 36, 46, 56, 87, 113, 62, 77, 96, 61, 81,
        115, 70, 79, 94, 75, 84, 124, 80, 95, 119, 92, 110, 120, 2, 20, 25, 26, 41, 3, 24,
        28, 39, 40, 42, 52, 58, 78, 116, 64, 100, 122, 71, 101, 121, 72, 106, 133, 83, 103, 127,
        88, 111, 129, 98, 108, 136, 4, 27, 37, 38, 48, 5, 22, 31, 43, 47, 49, 57, 63, 67,
        130, 73, 132, 82, 97, 99, 125, 91, 123, 107, 126, 112, 134, 17, 35, 44, 50, 53, 13, 29,
        32, 51, 54, 55, 59, 68, 76, 128, 93, 131, 89, 109, 102, 117, 104, 137, 118, 135, 114, 138,
        6, 7, 18, 14, 21, 8, 12, 15, 9, 45, 60, 65, 66, 69, 74, 85, 86, 90, 105,
    ),
}


def schedule(z_n, pairs, tiles):
    times = {}
    for p in range(pairs):
        at = 9.0 + 3.0 * p
        for s in range(2):
            times["P", p, s] = 0.01 * p if p < pairs - 1 else 9.1
            times["A", p, s] = at + 0.01 * s
            times["B1", p, s] = at + 0.1 + 0.01 * s
            times["B2", p, s] = at + 0.5 + 0.01 * s
            times["C", p, s] = at + 8.0 + 0.01 * s
        times["Z", p] = at + 8.1
        steps = (z_n - 1).bit_length()
        for b in range(1, steps):
            times["H", p, b] = at + 8.0 + 5.5 * b
        done = max(26.0 + 4.0 * p, at + 8.0 + 5.5 * steps)
        times["D", p] = done
        if p >= pairs - LATE:
            times["F", p] = done + 3.2
        for k in range(z_n):
            for d in range(2 if k else 1):
                if k:
                    times["E", p, k, d] = done + 3.5 * k
                if p < pairs - LATE:
                    times["R", p, k, d] = done + 3.5 * k + 3.2
                times["S", p, k, d] = done + 3.5 * k + 6.8
    times["mate",] = 0.005
    for s in range(2):
        times["hitO", s] = 2.0 + 0.1 * s
        times["hitN", s] = 4.6 + 0.1 * s
        times["own", s, 1] = 4.0 + 0.1 * s
        times["own", s, 0] = 4.3 + 0.1 * s
    for i in range(tiles):
        times["L", i] = 26.5 + 1.5 * i
    times["X",] = 27.0 + 1.5 * tiles
    times["Y",] = 33.0 + 1.5 * tiles
    tuned = TUNED.get((z_n, pairs, tiles))
    if tuned is not None:
        times = dict(zip(times, tuned, strict=True))
    return sorted(times, key=lambda task: times[task])


def update_kernel(
    z_n, pairs, p_hbm, c_hbm, assign_hbm, keep_hbm, code_hbm, cost_ref,
    out_ref, p2, cents, ak, prior, idv, slot, hit, pn, acc, cnt, asend, arecv, zsend, zrecv, low, lowr,
    loc, ids_s, ids_r, mt_s, mt_r, ps, pr, fs, fr, as_, ar, zs, zr,
    grs, grr, gls, glr, xs, xr, ys, yr, ds_, dr, outs, f1s, f1r, f2s, f2r, hrs, hrr, hls, hlr, lo_s, lo_r,
):
    z, q, m = lax.axis_index("z"), lax.axis_index("q"), lax.axis_index("mp")
    nx = q + 1 - 2 * lax.rem(q, 2)
    ny = lax.rem(q + 2, PLANE)
    other = 1 - m
    rows, width = p_hbm.shape
    shard_rows = c_hbm.shape[0]
    block = prior.shape[0]
    both = 2 * rows
    kept = z_n * block
    side_w = width // 2
    part = side_w // pairs
    last = z_n - 1
    bits = last.bit_length()
    up, down = lax.rem(z + 1, z_n), lax.rem(z + last, z_n)
    own = z * PLANE + q
    near, far = (nx, ny), (ny, nx)

    load_p = pltpu.make_async_copy(p_hbm, p2.at[pl.ds(0, rows)], loc.at[0])
    load_prior = pltpu.make_async_copy(
        c_hbm.at[pl.ds(pl.multiple_of(own * block, block), block)], prior, loc.at[1]
    )
    load_c = pltpu.make_async_copy(c_hbm, cents, loc.at[2])
    load_a = pltpu.make_async_copy(assign_hbm, ak.at[0], loc.at[3])
    load_k = pltpu.make_async_copy(keep_hbm, ak.at[1], loc.at[4])
    for copy in (load_a, load_k, load_p):
        copy.start()

    barrier = pltpu.get_barrier_semaphore()
    peers = [(z, q, other), (z, nx, m), (z, nx, other), (z, ny, m), (z, ny, other)]
    greet = peers + [(lax.rem(z + k, z_n), q, m) for k in range(1, z_n)]
    for peer in greet:
        pl.semaphore_signal(barrier, inc=1, device_id=peer, device_id_type=MESH)
    load_a.wait()
    load_k.wait()
    idv[0] = jnp.where(ak[1] > 0, ak[0], -1)
    load_c.start()
    load_prior.start()
    pl.semaphore_wait(barrier, len(greet))

    def pts_copy(s, p):
        cols = pl.ds(s * side_w + p * part, part)
        return remote(
            p2.at[pl.ds(0, rows), cols], pn.at[s, pl.ds(0, rows), pl.ds(p * part, part)], ps.at[s, p], pr.at[s, p],
            (z, near[s], m),
        )

    def fwd_copy(s, p):
        return remote(
            pn.at[s, pl.ds(0, rows), pl.ds(p * part, part)], pn.at[s, pl.ds(rows, rows), pl.ds(p * part, part)], fs.at[s, p], fr.at[s, p],
            (z, q, other),
        )

    def a_copy(s, p):
        return remote(asend.at[s, p], arecv.at[s, p], as_.at[s, p], ar.at[s, p], (z, far[s], m))

    def z_copy(p, b):
        n = z_n >> (b + 1)
        at = pl.ds(z_n - 2 * n, n)
        bit = lax.rem(lax.div(z, 1 << b), 2)
        to = z + (1 << b) * (1 - 2 * bit)
        return remote(zsend.at[p, at], zrecv.at[p, at], zs.at[p, b], zr.at[p, b], (to, q, m))

    id_copies = [
        remote(idv.at[0], idv.at[k + 1], ids_s.at[k], ids_r.at[k], peer) for k, peer in enumerate(peers)
    ]
    mate_copy = remote(p2.at[pl.ds(0, rows)], p2.at[pl.ds(rows, rows)], mt_s, mt_r, (z, q, other))

    load_p.wait()
    for copy in id_copies:
        copy.start()

    def slots_of(s, a, b):
        ids = jnp.concatenate([idv[a], idv[b]], axis=1) - m * shard_rows
        inside = (ids >= 0) & (ids < shard_rows)
        ids = jnp.where(inside, ids, 0)
        owner = lax.rem(lax.div(ids, block), PLANE)
        at = lax.div(ids, block * PLANE) * block + lax.rem(ids, block)
        found = jnp.where(owner == q, at, jnp.where(owner == far[s], at + kept, -1))
        return jnp.where(inside, found, -1)

    def fill_hits(s, first):
        group = s if first else 2 + s
        slot[s] = slots_of(s, *((0, 1) if first else ((2, 3), (4, 5))[s]))

        def tile(t, carry):
            base = pl.multiple_of(t * LANES, LANES)
            row = lax.broadcasted_iota(jnp.int32, (LANES, both), 0) + base
            hit[group, pl.ds(base, LANES), :] = jnp.where(row == slot[s], 1.0, 0.0).astype(jnp.bfloat16)
            return carry

        lax.fori_loop(0, 2 * kept // LANES, tile, 0)

    ones = jnp.ones((both, LANES), jnp.bfloat16)

    def own_dot(s, half):
        at = pl.ds(half * kept, kept)
        acc[s, at, :] = jnp.dot(
            hit[s, at, :], p2[:, s * side_w : (s + 1) * side_w], preferred_element_type=jnp.float32
        )
        if s == 0:
            cnt[at, :] = jnp.dot(hit[s, at, :], ones, preferred_element_type=jnp.float32)

    def near_dot(s, p, half):
        at, cols = pl.ds(half * kept, kept), pl.ds(p * part, part)
        points = pn[s, :, p * part : (p + 1) * part]
        if s == 0 and p == 0:
            points = jnp.concatenate([points, ones], axis=1)
        more = jnp.dot(hit[2 + s, at, :], points, preferred_element_type=jnp.float32)
        acc[s, at, cols] += more[:, :part]
        if s == 0 and p == 0:
            cnt[at, :] += more[:, part:]

    def rows_of(t):
        return pl.ds(pl.multiple_of(t * block, block), block)

    def half_rows_of(t):
        return pl.ds(pl.multiple_of(t * (block // 2), block // 2), block // 2)

    def step_a(p, s):
        pts_copy(s, p).wait_recv()
        fwd_copy(s, p).start()

    def step_b(p, s):
        fwd_copy(s, p).wait_recv()
        near_dot(s, p, 1)

        def tile(t, carry):
            at = pl.ds(pl.multiple_of(kept + t * block, block), block)
            count = cnt[at, 0:1] if s == 0 and p == 0 else None
            asend[s, p, half_rows_of(t), :] = encode(acc[s, at, p * part : (p + 1) * part], count)
            return carry

        lax.fori_loop(0, z_n, tile, 0)
        a_copy(s, p).start()

    def step_b2(p, s):
        near_dot(s, p, 0)

    def side_of(s):
        return slice(s * (block // 2), (s + 1) * (block // 2))

    def target(b, j, mine):
        bit = lax.rem(lax.div(z, 1 << b), 2)
        return j * (2 << b) + lax.rem(z, 1 << b) + (bit if mine else 1 - bit) * (1 << b)

    def z_send(p, b):
        n = z_n >> (b + 1)
        for s in range(2):
            def tile(j, carry, s=s):
                at = rows_of(target(b, j, False))
                count = cnt[at, 0:1] if s == 0 and p == 0 else None
                zsend[p, z_n - 2 * n + j, side_of(s), :] = encode(acc[s, at, p * part : (p + 1) * part], count)
                return carry

            lax.fori_loop(0, n, tile, 0)
        z_copy(p, b).start()

    def gain(s, p, at, packed):
        acc[s, at, p * part : (p + 1) * part] += decode(packed)
        if s == 0 and p == 0:
            cnt[at, :] = jnp.broadcast_to(cnt[at, 0:1] + count_of(unpack(packed)), (block, LANES))

    def step_c(p, s):
        a_copy(s, p).wait_recv()

        def tile(t, carry):
            gain(s, p, rows_of(t), arecv[s, p, half_rows_of(t), :])
            return carry

        lax.fori_loop(0, z_n, tile, 0)

    def z_gain(p, b):
        n = z_n >> (b + 1)
        z_copy(p, b).wait_recv()
        for s in range(2):
            def tile(j, carry, s=s):
                gain(s, p, rows_of(target(b, j, True)), zrecv[p, z_n - 2 * n + j, side_of(s), :])
                return carry

            lax.fori_loop(0, n, tile, 0)

    def step_h(p, b):
        z_gain(p, b - 1)
        z_send(p, b)

    def xcopy(p, n, to_q):
        at = out_ref.at[p, n * PLANE + to_q]
        return remote(at, at, xs.at[p, n], xr.at[p, n], (z, nx, m))

    def ycopy(p, n, to_q):
        at = out_ref.at[p, n * PLANE + to_q]
        return remote(at, at, ys.at[p, n], yr.at[p, n], (z, ny, m))

    def dcopy(p, n, by_x):
        at = out_ref.at[p, n * PLANE + (nx if by_x else ny)]
        return remote(at, at, ds_.at[p, n], dr.at[p, n], (z, ny if by_x else nx, m))

    def gright(p, n):
        at = out_ref.at[p, n * PLANE + q]
        return remote(at, at, grs.at[p, n], grr.at[p, n], (up, q, m))

    def gleft(p, n):
        at = out_ref.at[p, n * PLANE + q]
        return remote(at, at, gls.at[p, n], glr.at[p, n], (down, q, m))

    def late(p):
        return p >= pairs - LATE

    def first_copy(p, s):
        at = out_ref.at[p, own, side_of(s)]
        return remote(at, at, f1s.at[p, s], f1r.at[p, s], (z, near[s], m))

    def second_copy(p, n, s, j):
        at = out_ref.at[p, n * PLANE + (near[s] if j else q), side_of(s)]
        i = 2 * s + j
        return remote(at, at, f2s.at[p, n, i], f2r.at[p, n, i], (z, far[s], m))

    def hright(p, n, s):
        at = out_ref.at[p, n * PLANE + near[s], side_of(s)]
        return remote(at, at, hrs.at[p, n, s], hrr.at[p, n, s], (up, q, m))

    def hleft(p, n, s):
        at = out_ref.at[p, n * PLANE + near[s], side_of(s)]
        return remote(at, at, hls.at[p, n, s], hlr.at[p, n, s], (down, q, m))

    def step_f(p):
        for s in range(2):
            first_copy(p, s).wait_recv()

        @pl.when(z < last)
        def _():
            for s in range(2):
                hright(p, z, s).start()

        @pl.when(z > 0)
        def _():
            for s in range(2):
                hleft(p, z, s).start()

        for s in range(2):
            second_copy(p, z, s, 1).start()

    def step_d(p):
        mine = rows_of(z)
        z_gain(p, bits - 1)
        if p == 0:
            load_prior.wait()
        count = cnt[mine, 0:1]
        fresh = []
        for s in range(2):
            lo = s * side_w + p * part
            total = acc[s, mine, p * part : (p + 1) * part]
            fallback = prior[:, lo : lo + part].astype(jnp.float32)
            fresh.append(jnp.where(count > 0.5, total / jnp.maximum(count, 1.0), fallback))
        for s in range(2):
            out_ref[p, own, side_of(s)] = publish_code(fresh[s])

        @pl.when(z < last)
        def _():
            gright(p, z).start()

        @pl.when(z > 0)
        def _():
            gleft(p, z).start()

        if late(p):
            for s in range(2):
                first_copy(p, s).start()
            for s in range(2):
                second_copy(p, z, s, 0).start()
            return

        xcopy(p, z, q).start()
        ycopy(p, z, q).start()

    def relay(p, n, by_x):
        if by_x:
            xcopy(p, n, nx).wait_recv()
        else:
            ycopy(p, n, ny).wait_recv()
        dcopy(p, n, by_x).start()

    def settle(p, n, by_x):
        if late(p):
            for s in range(2):
                for j in range(2):
                    second_copy(p, n, s, j).wait_recv()
            put(p, n).start()
            return
        if by_x:
            ycopy(p, n, ny).wait_recv()
        else:
            xcopy(p, n, nx).wait_recv()
        dcopy(p, n, by_x).wait_recv()

        put(p, n).start()

    def put(p, n):
        at = pl.ds(n * PLANE, PLANE)
        return pltpu.make_async_copy(out_ref.at[p, at], code_hbm.at[p, at], outs.at[p, n])

    def each(p, k, d, action):
        if k == 0:
            action(p, z, p % 2 == 0)
            return

        @pl.when((z >= k) if d == 0 else (z + k <= last))
        def _():
            action(p, z - k if d == 0 else z + k, (k + p) % 2 == d)

    def spread(p, k, d):
        @pl.when((z >= k) if d == 0 else (z + k <= last))
        def _():
            n, hop = (z - k, gright) if d == 0 else (z + k, gleft)
            hop(p, n).wait_recv()

            @pl.when((z < last) if d == 0 else (z > 0))
            def _():
                hop(p, n).start()

            if not late(p):
                xcopy(p, n, q).start()
                ycopy(p, n, q).start()
                return

            for s in range(2):
                second_copy(p, n, s, 0).start()
            hops = hright if d == 0 else hleft
            for s in range(2):
                hops(p, n, s).wait_recv()

            @pl.when((z < last) if d == 0 else (z > 0))
            def _():
                for s in range(2):
                    hops(p, n, s).start()

            for s in range(2):
                second_copy(p, n, s, 1).start()

    met = []

    def meet():
        if not met:
            met.append(True)
            mate_copy.wait_recv()

    seen = []

    def lowest():
        i = len(seen)
        seen.append(i)
        meet()
        if i == 0:
            load_c.wait()

        def tile(t, best):
            tile_ref = cents[pl.ds(pl.multiple_of(t * CTILE, CTILE), CTILE), :]
            wide = tile_ref.astype(jnp.float32)
            sq = jnp.sum(wide * wide, axis=1, keepdims=True)
            inner = lax.dot_general(
                tile_ref, p2[...], (((1,), (1,)), ((), ())), preferred_element_type=jnp.float32
            )
            return jnp.minimum(best, jnp.min(sq - 2.0 * inner, axis=0, keepdims=True))

        start = jnp.full((1, both), jnp.inf, jnp.float32) if i == 0 else low[...]
        low[...] = lax.fori_loop(i, i + 1, tile, start)

    low_copy = remote(low.at[:, pl.ds(rows, rows)], lowr, lo_s, lo_r, (z, q, other))

    def finish_cost():
        low_copy.wait_recv()
        wide = p2[pl.ds(0, rows), :].astype(jnp.float32)
        sq = jnp.sum(wide * wide, axis=1, keepdims=True)
        flat = jnp.broadcast_to(sq, (rows, LANES)).T[0:1, :]
        cost_ref[...] = (flat + jnp.minimum(low[:, :rows], lowr[...])) / width

    greeted = []

    def hits(s, first):
        if not greeted:
            greeted.append(True)
            for copy in id_copies:
                copy.wait_recv()
        fill_hits(s, first)

    def own_part(s, half):
        meet()
        own_dot(s, half)

    actions = {
        "P": lambda p, s: pts_copy(s, p).start(), "mate": mate_copy.start,
        "hitO": lambda s: hits(s, True), "hitN": lambda s: hits(s, False), "own": own_part,
        "A": step_a, "B1": step_b, "B2": step_b2, "C": step_c, "Z": lambda p: z_send(p, 0), "H": step_h,
        "D": step_d, "F": step_f, "E": spread, "R": lambda p, k, d: each(p, k, d, relay),
        "S": lambda p, k, d: each(p, k, d, settle), "L": lambda i: lowest(),
        "X": low_copy.start, "Y": finish_cost,
    }
    for task in schedule(z_n, pairs, shard_rows // CTILE):
        actions[task[0]](*task[1:])

    for copy in id_copies + [mate_copy, low_copy]:
        copy.wait_send()
    for p in range(pairs):
        for s in range(2):
            if late(p):
                first_copy(p, s).wait_send()
            pts_copy(s, p).wait_send()
            fwd_copy(s, p).wait_send()
            a_copy(s, p).wait_send()
        for t in range(z_n):
            if t < bits:
                z_copy(p, t).wait_send()

            @pl.when((z >= t) & (z < last))
            def _(p=p, t=t):
                gright(p, t).wait_send()
                if late(p):
                    for s in range(2):
                        hright(p, t, s).wait_send()

            @pl.when((z <= t) & (z > 0))
            def _(p=p, t=t):
                gleft(p, t).wait_send()
                if late(p):
                    for s in range(2):
                        hleft(p, t, s).wait_send()

            put(p, t).wait()
            if late(p):
                for s in range(2):
                    for j in range(2):
                        second_copy(p, t, s, j).wait_send()
                continue
            xcopy(p, t, q).wait_send()
            ycopy(p, t, q).wait_send()
            dcopy(p, t, True).wait_send()


def decode_kernel(in_hbm, cost_in, out_hbm, cost_out, codes, fresh, cost, ins, outs, row):
    pairs, dp_n, block, part = codes.shape
    half = block // 2
    size = group_of(half)
    side_w = fresh.shape[1] // 2
    lane = lax.broadcasted_iota(jnp.int32, (1, LANES), 1)
    weight = jnp.where(lane < FINE_BITS, 1 << jnp.minimum(lane, FINE_BITS), 0).astype(jnp.float32)
    owners = max(1, min(dp_n, 256 // block))

    def load(i):
        at = pl.ds(i * owners, owners)
        return pltpu.make_async_copy(in_hbm.at[:, at], codes.at[:, at], ins.at[i])

    def store(i):
        at = pl.ds(i * owners * block, owners * block)
        return pltpu.make_async_copy(fresh.at[at], out_hbm.at[at], outs.at[i])

    for i in range(dp_n // owners):
        load(i).start()
    take = pltpu.make_async_copy(cost_in, cost, row.at[0])
    give = pltpu.make_async_copy(cost, cost_out, row.at[1])
    take.start()

    def owner(o, carry):
        for p in range(pairs):
            for s in range(2):
                cols = slice(s * side_w + p * part, s * side_w + (p + 1) * part)
                for g in range(half // size):
                    packed = codes[p, o, s * half + g * size : s * half + (g + 1) * size]
                    bits = ((packed[:8] >> 16) & 1).astype(jnp.float32)
                    word = jnp.sum(bits * weight, axis=1, keepdims=True) - FINE_BIAS
                    scale = jnp.exp2(word * (1.0 / FINE)) * (1.0 / STEPS)
                    scale = jnp.broadcast_to(scale[0:1], (1, part))
                    at = pl.multiple_of(o * block, block) + g * size
                    fresh[pl.ds(at, size), cols] = (packed >> 16).astype(jnp.float32) * scale
                    low = ((packed << 16) >> 16).astype(jnp.float32)
                    fresh[pl.ds(at + half, size), cols] = low * scale
        return carry

    for i in range(dp_n // owners):
        load(i).wait()
        lax.fori_loop(i * owners, (i + 1) * owners, owner, 0)
        store(i).start()
    take.wait()
    give.start()
    for i in range(dp_n // owners):
        store(i).wait()
    give.wait()


def shards(points, centroids, assign, keep_mask):
    rows, width = points.shape
    shard_rows = centroids.shape[0]
    z_n = lax.axis_size("z")
    dp_n = z_n * PLANE
    block = shard_rows // dp_n
    kept = z_n * block
    part = LANES
    side_w = width // 2
    pairs = side_w // part
    vmem = pl.BlockSpec(memory_space=pltpu.VMEM)
    hbm = pl.BlockSpec(memory_space=pltpu.HBM)
    dma = pltpu.SemaphoreType.DMA
    by_pair = dma((2, pairs))
    by_z = dma((pairs, z_n))
    halves = dma((pairs, 2))
    by_half = dma((pairs, z_n, 2))
    by_quarter = dma((pairs, z_n, 4))
    codes, cost = pl.pallas_call(
        functools.partial(update_kernel, z_n, pairs),
        out_shape=(
            jax.ShapeDtypeStruct((pairs, dp_n, block, part), jnp.int32),
            jax.ShapeDtypeStruct((1, rows), jnp.float32),
        ),
        in_specs=[hbm] * 4,
        out_specs=(hbm, vmem),
        scratch_shapes=[
            pltpu.VMEM((pairs, dp_n, block, part), jnp.int32),
            pltpu.VMEM((2 * rows, width), points.dtype),
            pltpu.VMEM((shard_rows, width), centroids.dtype),
            pltpu.VMEM((2, 1, rows), jnp.int32),
            pltpu.VMEM((block, width), centroids.dtype),
            pltpu.VMEM((6, 1, rows), jnp.int32),
            pltpu.VMEM((2, 1, 2 * rows), jnp.int32),
            pltpu.VMEM((4, 2 * kept, 2 * rows), jnp.bfloat16),
            pltpu.VMEM((2, 2 * rows, side_w), points.dtype),
            pltpu.VMEM((2, 2 * kept, side_w), jnp.float32),
            pltpu.VMEM((2 * kept, LANES), jnp.float32),
            pltpu.VMEM((2, pairs, kept // 2, part), jnp.int32),
            pltpu.VMEM((2, pairs, kept // 2, part), jnp.int32),
            pltpu.VMEM((pairs, z_n, block, part), jnp.int32),
            pltpu.VMEM((pairs, z_n, block, part), jnp.int32),
            pltpu.VMEM((1, 2 * rows), jnp.float32),
            pltpu.VMEM((1, rows), jnp.float32),
            dma((5,)), dma((5,)), dma((5,)), dma, dma,
            by_pair, by_pair, by_pair, by_pair, by_pair, by_pair,
            by_z, by_z, by_z, by_z, by_z, by_z, by_z, by_z, by_z, by_z, by_z, by_z, by_z,
            halves, halves, by_quarter, by_quarter, by_half, by_half, by_half, by_half,
            dma, dma,
        ],
        compiler_params=pltpu.CompilerParams(
            collective_id=0, has_side_effects=True, vmem_limit_bytes=56 * 1024 * 1024
        ),
        cost_estimate=pl.CostEstimate(
            flops=0, bytes_accessed=200 * 1024 * 1024, transcendentals=0
        ),
        name="update",
    )(points, centroids, assign.reshape(1, rows), keep_mask.reshape(1, rows))
    new_centroids, cost = pl.pallas_call(
        decode_kernel,
        in_specs=[hbm, hbm],
        out_specs=(hbm, hbm),
        out_shape=(
            jax.ShapeDtypeStruct((shard_rows, width), jnp.float32),
            jax.ShapeDtypeStruct((1, rows), jnp.float32),
        ),
        scratch_shapes=[
            pltpu.VMEM((pairs, dp_n, block, part), jnp.int32),
            pltpu.VMEM((shard_rows, width), jnp.float32),
            pltpu.VMEM((1, rows), jnp.float32),
            dma((dp_n,)), dma((dp_n,)), dma((2,)),
        ],
        compiler_params=pltpu.CompilerParams(vmem_limit_bytes=56 * 1024 * 1024),
        name="decode",
    )(codes, cost)
    return new_centroids, cost.reshape(rows)


def solution(mesh):
    dp, mp = mesh.shape["dp"], mesh.shape["mp"]
    grid = Mesh(mesh.devices.reshape(dp // PLANE, PLANE, mp), ("z", "q", "mp"))
    rows = ("z", "q", "mp")
    in_specs = (P(rows, None), P("mp", None), P(rows), P(rows))
    out_specs = (P("mp", None), P(rows))
    return jax.shard_map(shards, mesh=grid, in_specs=in_specs, out_specs=out_specs, check_vma=False)
```

```python
import functools

import jax
import jax.numpy as jnp
from jax import lax
from jax.experimental import pallas as pl
from jax.experimental.pallas import tpu as pltpu
from jax.sharding import Mesh
from jax.sharding import PartitionSpec as P

STEPS = 32000.0
TINY = 2.0**-100
BIAS = 128
EXP = 8
WORD = 32
GROUP = 16
FINE = 8.0
FINE_BIAS = 1024
FINE_BITS = 12
PLANE = 4
LATE = 2
LANES = 128
CTILE = 256
MESH = pl.DeviceIdType.MESH


def remote(src, dst, send, recv, device):
    return pltpu.make_async_remote_copy(
        src_ref=src, dst_ref=dst, send_sem=send, recv_sem=recv, device_id=device, device_id_type=MESH
    )


def power_of(top):
    return jnp.ceil(jnp.log2(jnp.maximum(top, TINY)))


def quantize(v, power):
    return jnp.floor(v * (jnp.exp2(-power) * STEPS) + 0.5).astype(jnp.int32)


def embed(code, power, count=None):
    lane = lax.broadcasted_iota(jnp.int32, code.shape, 1)
    bit = lax.shift_right_logical(jnp.broadcast_to(power, code.shape), jnp.minimum(lane, 31)) & 1
    used = EXP
    if count is not None:
        at = jnp.clip(lane - EXP, 0, 31)
        bit = jnp.where(lane < EXP, bit, lax.shift_right_logical(jnp.broadcast_to(count, code.shape), at) & 1)
        used = WORD
    return (code & jnp.where(lane < used, -2, -1)) | bit


def pack(code):
    half = code.shape[0] // 2
    return (code[:half] << 16) | (code[half:] & 0xFFFF)


def unpack(packed):
    return jnp.concatenate([packed >> 16, (packed << 16) >> 16], axis=0)


def bits_word(code, lo, hi):
    lane = lax.broadcasted_iota(jnp.int32, (1, LANES), 1)
    weight = jnp.where((lane >= lo) & (lane < hi), 1 << jnp.clip(lane - lo, 0, hi - lo), 0)
    bits = (code[:, :LANES] & 1).astype(jnp.float32)
    return jnp.sum(bits * weight.astype(jnp.float32), axis=1, keepdims=True)


def scale_of(code):
    return jnp.exp2(bits_word(code, 0, EXP) - BIAS) * (1.0 / STEPS)


def count_of(code):
    return bits_word(code, EXP, WORD)


def encode(v, count=None):
    power = power_of(jnp.max(jnp.abs(v), axis=1, keepdims=True))
    if count is not None:
        count = count.astype(jnp.int32)
    return pack(embed(quantize(v, power), power.astype(jnp.int32) + BIAS, count))


def decode(packed):
    code = unpack(packed)
    return code.astype(jnp.float32) * scale_of(code)


def group_of(half):
    return min(GROUP, half)


def publish_code(v):
    half = v.shape[0] // 2
    size = group_of(half)
    lane = lax.broadcasted_iota(jnp.int32, (size, LANES), 1)
    out = []
    for g in range(half // size):
        hi, lo = v[g * size : (g + 1) * size], v[half + g * size : half + (g + 1) * size]
        top = jnp.max(jnp.maximum(jnp.abs(hi), jnp.abs(lo)), axis=0, keepdims=True)
        top = jnp.maximum(jnp.max(top, axis=1, keepdims=True), TINY)
        word = jnp.ceil(jnp.log2(top) * FINE)
        factor = jnp.exp2(word * (-1.0 / FINE)) * STEPS
        codes = [jnp.floor(part * factor + 0.5).astype(jnp.int32) for part in (hi, lo)]
        bit = lax.shift_right_logical(
            jnp.broadcast_to(word.astype(jnp.int32) + FINE_BIAS, (size, LANES)), jnp.minimum(lane, 31)
        ) & 1
        first = (codes[0] & jnp.where(lane < FINE_BITS, -2, -1)) | jnp.where(lane < FINE_BITS, bit, 0)
        out.append((first << 16) | (codes[1] & 0xFFFF))
    return jnp.concatenate(out, axis=0)


TUNED = {
    (4, 4, 8): (
        2, 16, 19, 25, 32, 1, 12, 17, 21, 30, 34, 42, 31, 45, 55, 68, 94, 67, 85, 118,
        66, 110, 134, 80, 89, 137, 75, 124, 138, 90, 99, 127, 79, 101, 125, 3, 20, 23, 35, 39,
        4, 18, 22, 26, 37, 41, 51, 38, 49, 60, 70, 140, 72, 96, 115, 73, 87, 116, 81, 111,
        136, 82, 119, 133, 95, 102, 109, 93, 108, 141, 28, 44, 53, 57, 61, 33, 52, 54, 62, 63,
        65, 77, 64, 76, 84, 97, 122, 100, 144, 104, 128, 106, 135, 123, 143, 114, 146, 131, 145, 9,
        24, 27, 43, 46, 13, 29, 36, 40, 48, 47, 59, 50, 58, 71, 78, 126, 88, 121, 91, 120,
        103, 130, 98, 139, 107, 142, 112, 129, 0, 5, 6, 7, 11, 10, 8, 14, 15, 56, 69, 74,
        83, 86, 92, 105, 113, 117, 132,
    ),
}


def schedule(z_n, pairs, tiles):
    times = {}
    for p in range(pairs):
        at = 9.0 + 3.0 * p
        for s in range(2):
            times["P", p, s] = 0.01 * p if p < pairs - 1 else 9.1
            times["A", p, s] = at + 0.01 * s
            times["B1", p, s] = at + 0.1 + 0.01 * s
            times["B2", p, s] = at + 0.5 + 0.01 * s
            times["C", p, s] = at + 8.0 + 0.01 * s
        steps = (z_n - 1).bit_length()
        for s in range(2):
            times["Z", p, s] = at + 8.1 + 0.01 * s
            for b in range(1, steps):
                times["H", p, b, s] = at + 8.0 + 5.5 * b + 0.01 * s
        done = max(26.0 + 4.0 * p, at + 8.0 + 5.5 * steps)
        times["D", p] = done
        if p >= pairs - LATE:
            times["F", p] = done + 3.2
        for k in range(z_n):
            for d in range(2 if k else 1):
                if k:
                    times["E", p, k, d] = done + 3.5 * k
                if p < pairs - LATE:
                    times["R", p, k, d] = done + 3.5 * k + 3.2
                times["S", p, k, d] = done + 3.5 * k + 6.8
    times["mate",] = 0.005
    for s in range(2):
        times["hitO", s] = 2.0 + 0.1 * s
        times["hitN", s] = 4.6 + 0.1 * s
        times["own", s, 1] = 4.0 + 0.1 * s
        times["own", s, 0] = 4.3 + 0.1 * s
    for i in range(tiles):
        times["L", i] = 26.5 + 1.5 * i
    times["X",] = 27.0 + 1.5 * tiles
    times["Y",] = 33.0 + 1.5 * tiles
    tuned = TUNED.get((z_n, pairs, tiles))
    if tuned is not None:
        times = dict(zip(times, tuned, strict=True))
    return sorted(times, key=lambda task: times[task])


def update_kernel(
    z_n, pairs, p_hbm, c_hbm, assign_hbm, keep_hbm, code_hbm, cost_ref,
    out_ref, p2, cents, ak, prior, idv, slot, hit, pn, acc, cnt, asend, arecv, zsend, zrecv, low, lowr,
    loc, ids_s, ids_r, mt_s, mt_r, ps, pr, fs, fr, as_, ar, zs, zr,
    grs, grr, gls, glr, xs, xr, ys, yr, ds_, dr, outs, f1s, f1r, f2s, f2r, hrs, hrr, hls, hlr, lo_s, lo_r,
):
    z, q, m = lax.axis_index("z"), lax.axis_index("q"), lax.axis_index("mp")
    nx = q + 1 - 2 * lax.rem(q, 2)
    ny = lax.rem(q + 2, PLANE)
    other = 1 - m
    rows, width = p_hbm.shape
    shard_rows = c_hbm.shape[0]
    block = prior.shape[0]
    both = 2 * rows
    kept = z_n * block
    side_w = width // 2
    part = side_w // pairs
    last = z_n - 1
    bits = last.bit_length()
    up, down = lax.rem(z + 1, z_n), lax.rem(z + last, z_n)
    own = z * PLANE + q
    near, far = (nx, ny), (ny, nx)

    load_p = pltpu.make_async_copy(p_hbm, p2.at[pl.ds(0, rows)], loc.at[0])
    load_prior = pltpu.make_async_copy(
        c_hbm.at[pl.ds(pl.multiple_of(own * block, block), block)], prior, loc.at[1]
    )
    load_c = pltpu.make_async_copy(c_hbm, cents, loc.at[2])
    load_a = pltpu.make_async_copy(assign_hbm, ak.at[0], loc.at[3])
    load_k = pltpu.make_async_copy(keep_hbm, ak.at[1], loc.at[4])
    for copy in (load_a, load_k, load_p):
        copy.start()

    barrier = pltpu.get_barrier_semaphore()
    peers = [(z, q, other), (z, nx, m), (z, nx, other), (z, ny, m), (z, ny, other)]
    greet = peers + [(lax.rem(z + k, z_n), q, m) for k in range(1, z_n)]
    for peer in greet:
        pl.semaphore_signal(barrier, inc=1, device_id=peer, device_id_type=MESH)
    load_a.wait()
    load_k.wait()
    idv[0] = jnp.where(ak[1] > 0, ak[0], -1)
    load_c.start()
    load_prior.start()
    pl.semaphore_wait(barrier, len(greet))

    def pts_copy(s, p):
        cols = pl.ds(s * side_w + p * part, part)
        return remote(
            p2.at[pl.ds(0, rows), cols], pn.at[s, pl.ds(0, rows), pl.ds(p * part, part)], ps.at[s, p], pr.at[s, p],
            (z, near[s], m),
        )

    def fwd_copy(s, p):
        return remote(
            pn.at[s, pl.ds(0, rows), pl.ds(p * part, part)], pn.at[s, pl.ds(rows, rows), pl.ds(p * part, part)], fs.at[s, p], fr.at[s, p],
            (z, q, other),
        )

    def a_copy(s, p):
        return remote(asend.at[s, p], arecv.at[s, p], as_.at[s, p], ar.at[s, p], (z, far[s], m))

    def side_of(s):
        return slice(s * (block // 2), (s + 1) * (block // 2))

    def z_copy(p, b, s):
        n = z_n >> (b + 1)
        at = pl.ds(z_n - 2 * n, n)
        bit = lax.rem(lax.div(z, 1 << b), 2)
        to = z + (1 << b) * (1 - 2 * bit)
        return remote(
            zsend.at[p, at, side_of(s)], zrecv.at[p, at, side_of(s)], zs.at[p, b, s], zr.at[p, b, s], (to, q, m)
        )

    id_copies = [
        remote(idv.at[0], idv.at[k + 1], ids_s.at[k], ids_r.at[k], peer) for k, peer in enumerate(peers)
    ]
    mate_copy = remote(p2.at[pl.ds(0, rows)], p2.at[pl.ds(rows, rows)], mt_s, mt_r, (z, q, other))

    load_p.wait()
    for copy in id_copies:
        copy.start()

    def slots_of(s, a, b):
        ids = jnp.concatenate([idv[a], idv[b]], axis=1) - m * shard_rows
        inside = (ids >= 0) & (ids < shard_rows)
        ids = jnp.where(inside, ids, 0)
        owner = lax.rem(lax.div(ids, block), PLANE)
        at = lax.div(ids, block * PLANE) * block + lax.rem(ids, block)
        found = jnp.where(owner == q, at, jnp.where(owner == far[s], at + kept, -1))
        return jnp.where(inside, found, -1)

    def fill_hits(s, first):
        group = s if first else 2 + s
        slot[s] = slots_of(s, *((0, 1) if first else ((2, 3), (4, 5))[s]))

        def tile(t, carry):
            base = pl.multiple_of(t * LANES, LANES)
            row = lax.broadcasted_iota(jnp.int32, (LANES, both), 0) + base
            hit[group, pl.ds(base, LANES), :] = jnp.where(row == slot[s], 1.0, 0.0).astype(jnp.bfloat16)
            return carry

        lax.fori_loop(0, 2 * kept // LANES, tile, 0)

    ones = jnp.ones((both, LANES), jnp.bfloat16)

    def own_dot(s, half):
        at = pl.ds(half * kept, kept)
        acc[s, at, :] = jnp.dot(
            hit[s, at, :], p2[:, s * side_w : (s + 1) * side_w], preferred_element_type=jnp.float32
        )
        if s == 0:
            cnt[at, :] = jnp.dot(hit[s, at, :], ones, preferred_element_type=jnp.float32)

    def near_dot(s, p, half):
        at, cols = pl.ds(half * kept, kept), pl.ds(p * part, part)
        points = pn[s, :, p * part : (p + 1) * part]
        if s == 0 and p == 0:
            points = jnp.concatenate([points, ones], axis=1)
        more = jnp.dot(hit[2 + s, at, :], points, preferred_element_type=jnp.float32)
        acc[s, at, cols] += more[:, :part]
        if s == 0 and p == 0:
            cnt[at, :] += more[:, part:]

    def rows_of(t):
        return pl.ds(pl.multiple_of(t * block, block), block)

    def half_rows_of(t):
        return pl.ds(pl.multiple_of(t * (block // 2), block // 2), block // 2)

    def step_a(p, s):
        pts_copy(s, p).wait_recv()
        fwd_copy(s, p).start()

    def step_b(p, s):
        fwd_copy(s, p).wait_recv()
        near_dot(s, p, 1)

        def tile(t, carry):
            at = pl.ds(pl.multiple_of(kept + t * block, block), block)
            count = cnt[at, 0:1] if s == 0 and p == 0 else None
            asend[s, p, half_rows_of(t), :] = encode(acc[s, at, p * part : (p + 1) * part], count)
            return carry

        lax.fori_loop(0, z_n, tile, 0)
        a_copy(s, p).start()

    def step_b2(p, s):
        near_dot(s, p, 0)

    def target(b, j, mine):
        bit = lax.rem(lax.div(z, 1 << b), 2)
        return j * (2 << b) + lax.rem(z, 1 << b) + (bit if mine else 1 - bit) * (1 << b)

    def z_send(p, b, s):
        n = z_n >> (b + 1)

        def tile(j, carry):
            at = rows_of(target(b, j, False))
            count = cnt[at, 0:1] if s == 0 and p == 0 else None
            zsend[p, z_n - 2 * n + j, side_of(s), :] = encode(acc[s, at, p * part : (p + 1) * part], count)
            return carry

        lax.fori_loop(0, n, tile, 0)
        z_copy(p, b, s).start()

    def gain(s, p, at, packed):
        acc[s, at, p * part : (p + 1) * part] += decode(packed)
        if s == 0 and p == 0:
            cnt[at, :] = jnp.broadcast_to(cnt[at, 0:1] + count_of(unpack(packed)), (block, LANES))

    def step_c(p, s):
        a_copy(s, p).wait_recv()

        def tile(t, carry):
            gain(s, p, rows_of(t), arecv[s, p, half_rows_of(t), :])
            return carry

        lax.fori_loop(0, z_n, tile, 0)

    def z_gain(p, b, s):
        n = z_n >> (b + 1)
        z_copy(p, b, s).wait_recv()

        def tile(j, carry):
            gain(s, p, rows_of(target(b, j, True)), zrecv[p, z_n - 2 * n + j, side_of(s), :])
            return carry

        lax.fori_loop(0, n, tile, 0)

    def step_h(p, b, s):
        z_gain(p, b - 1, s)
        z_send(p, b, s)

    def xcopy(p, n, to_q):
        at = out_ref.at[p, n * PLANE + to_q]
        return remote(at, at, xs.at[p, n], xr.at[p, n], (z, nx, m))

    def ycopy(p, n, to_q):
        at = out_ref.at[p, n * PLANE + to_q]
        return remote(at, at, ys.at[p, n], yr.at[p, n], (z, ny, m))

    def dcopy(p, n, by_x):
        at = out_ref.at[p, n * PLANE + (nx if by_x else ny)]
        return remote(at, at, ds_.at[p, n], dr.at[p, n], (z, ny if by_x else nx, m))

    def gright(p, n):
        at = out_ref.at[p, n * PLANE + q]
        return remote(at, at, grs.at[p, n], grr.at[p, n], (up, q, m))

    def gleft(p, n):
        at = out_ref.at[p, n * PLANE + q]
        return remote(at, at, gls.at[p, n], glr.at[p, n], (down, q, m))

    def late(p):
        return p >= pairs - LATE

    def first_copy(p, s):
        at = out_ref.at[p, own, side_of(s)]
        return remote(at, at, f1s.at[p, s], f1r.at[p, s], (z, near[s], m))

    def second_copy(p, n, s, j):
        at = out_ref.at[p, n * PLANE + (near[s] if j else q), side_of(s)]
        i = 2 * s + j
        return remote(at, at, f2s.at[p, n, i], f2r.at[p, n, i], (z, far[s], m))

    def hright(p, n, s):
        at = out_ref.at[p, n * PLANE + near[s], side_of(s)]
        return remote(at, at, hrs.at[p, n, s], hrr.at[p, n, s], (up, q, m))

    def hleft(p, n, s):
        at = out_ref.at[p, n * PLANE + near[s], side_of(s)]
        return remote(at, at, hls.at[p, n, s], hlr.at[p, n, s], (down, q, m))

    def step_f(p):
        for s in range(2):
            first_copy(p, s).wait_recv()

        @pl.when(z < last)
        def _():
            for s in range(2):
                hright(p, z, s).start()

        @pl.when(z > 0)
        def _():
            for s in range(2):
                hleft(p, z, s).start()

        for s in range(2):
            second_copy(p, z, s, 1).start()

    def step_d(p):
        mine = rows_of(z)
        for s in range(2):
            z_gain(p, bits - 1, s)
        if p == 0:
            load_prior.wait()
        count = cnt[mine, 0:1]
        fresh = []
        for s in range(2):
            lo = s * side_w + p * part
            total = acc[s, mine, p * part : (p + 1) * part]
            fallback = prior[:, lo : lo + part].astype(jnp.float32)
            fresh.append(jnp.where(count > 0.5, total / jnp.maximum(count, 1.0), fallback))
        for s in range(2):
            out_ref[p, own, side_of(s)] = publish_code(fresh[s])

        @pl.when(z < last)
        def _():
            gright(p, z).start()

        @pl.when(z > 0)
        def _():
            gleft(p, z).start()

        if late(p):
            for s in range(2):
                first_copy(p, s).start()
            for s in range(2):
                second_copy(p, z, s, 0).start()
            return

        xcopy(p, z, q).start()
        ycopy(p, z, q).start()

    def relay(p, n, by_x):
        if by_x:
            xcopy(p, n, nx).wait_recv()
        else:
            ycopy(p, n, ny).wait_recv()
        dcopy(p, n, by_x).start()

    def settle(p, n, by_x):
        if late(p):
            for s in range(2):
                for j in range(2):
                    second_copy(p, n, s, j).wait_recv()
            put(p, n).start()
            return
        if by_x:
            ycopy(p, n, ny).wait_recv()
        else:
            xcopy(p, n, nx).wait_recv()
        dcopy(p, n, by_x).wait_recv()

        put(p, n).start()

    def put(p, n):
        at = pl.ds(n * PLANE, PLANE)
        return pltpu.make_async_copy(out_ref.at[p, at], code_hbm.at[p, at], outs.at[p, n])

    def each(p, k, d, action):
        if k == 0:
            action(p, z, p % 2 == 0)
            return

        @pl.when((z >= k) if d == 0 else (z + k <= last))
        def _():
            action(p, z - k if d == 0 else z + k, (k + p) % 2 == d)

    def spread(p, k, d):
        @pl.when((z >= k) if d == 0 else (z + k <= last))
        def _():
            n, hop = (z - k, gright) if d == 0 else (z + k, gleft)
            hop(p, n).wait_recv()

            @pl.when((z < last) if d == 0 else (z > 0))
            def _():
                hop(p, n).start()

            if not late(p):
                xcopy(p, n, q).start()
                ycopy(p, n, q).start()
                return

            for s in range(2):
                second_copy(p, n, s, 0).start()
            hops = hright if d == 0 else hleft
            for s in range(2):
                hops(p, n, s).wait_recv()

            @pl.when((z < last) if d == 0 else (z > 0))
            def _():
                for s in range(2):
                    hops(p, n, s).start()

            for s in range(2):
                second_copy(p, n, s, 1).start()

    met = []

    def meet():
        if not met:
            met.append(True)
            mate_copy.wait_recv()

    seen = []

    def lowest():
        i = len(seen)
        seen.append(i)
        meet()
        if i == 0:
            load_c.wait()

        def tile(t, best):
            tile_ref = cents[pl.ds(pl.multiple_of(t * CTILE, CTILE), CTILE), :]
            wide = tile_ref.astype(jnp.float32)
            sq = jnp.sum(wide * wide, axis=1, keepdims=True)
            inner = lax.dot_general(
                tile_ref, p2[...], (((1,), (1,)), ((), ())), preferred_element_type=jnp.float32
            )
            return jnp.minimum(best, jnp.min(sq - 2.0 * inner, axis=0, keepdims=True))

        start = jnp.full((1, both), jnp.inf, jnp.float32) if i == 0 else low[...]
        low[...] = lax.fori_loop(i, i + 1, tile, start)

    low_copy = remote(low.at[:, pl.ds(rows, rows)], lowr, lo_s, lo_r, (z, q, other))

    def finish_cost():
        low_copy.wait_recv()
        wide = p2[pl.ds(0, rows), :].astype(jnp.float32)
        sq = jnp.sum(wide * wide, axis=1, keepdims=True)
        flat = jnp.broadcast_to(sq, (rows, LANES)).T[0:1, :]
        cost_ref[...] = (flat + jnp.minimum(low[:, :rows], lowr[...])) / width

    greeted = []

    def hits(s, first):
        if not greeted:
            greeted.append(True)
            for copy in id_copies:
                copy.wait_recv()
        fill_hits(s, first)

    def own_part(s, half):
        meet()
        own_dot(s, half)

    actions = {
        "P": lambda p, s: pts_copy(s, p).start(), "mate": mate_copy.start,
        "hitO": lambda s: hits(s, True), "hitN": lambda s: hits(s, False), "own": own_part,
        "A": step_a, "B1": step_b, "B2": step_b2, "C": step_c, "Z": lambda p, s: z_send(p, 0, s), "H": step_h,
        "D": step_d, "F": step_f, "E": spread, "R": lambda p, k, d: each(p, k, d, relay),
        "S": lambda p, k, d: each(p, k, d, settle), "L": lambda i: lowest(),
        "X": low_copy.start, "Y": finish_cost,
    }
    for task in schedule(z_n, pairs, shard_rows // CTILE):
        actions[task[0]](*task[1:])

    for copy in id_copies + [mate_copy, low_copy]:
        copy.wait_send()
    for p in range(pairs):
        for s in range(2):
            if late(p):
                first_copy(p, s).wait_send()
            pts_copy(s, p).wait_send()
            fwd_copy(s, p).wait_send()
            a_copy(s, p).wait_send()
        for t in range(z_n):
            if t < bits:
                for s in range(2):
                    z_copy(p, t, s).wait_send()

            @pl.when((z >= t) & (z < last))
            def _(p=p, t=t):
                gright(p, t).wait_send()
                if late(p):
                    for s in range(2):
                        hright(p, t, s).wait_send()

            @pl.when((z <= t) & (z > 0))
            def _(p=p, t=t):
                gleft(p, t).wait_send()
                if late(p):
                    for s in range(2):
                        hleft(p, t, s).wait_send()

            put(p, t).wait()
            if late(p):
                for s in range(2):
                    for j in range(2):
                        second_copy(p, t, s, j).wait_send()
                continue
            xcopy(p, t, q).wait_send()
            ycopy(p, t, q).wait_send()
            dcopy(p, t, True).wait_send()


def decode_kernel(in_hbm, cost_in, out_hbm, cost_out, codes, fresh, cost, ins, outs, row):
    pairs, dp_n, block, part = codes.shape
    half = block // 2
    size = group_of(half)
    side_w = fresh.shape[1] // 2
    lane = lax.broadcasted_iota(jnp.int32, (1, LANES), 1)
    weight = jnp.where(lane < FINE_BITS, 1 << jnp.minimum(lane, FINE_BITS), 0).astype(jnp.float32)
    owners = max(1, min(dp_n, 256 // block))

    def load(i):
        at = pl.ds(i * owners, owners)
        return pltpu.make_async_copy(in_hbm.at[:, at], codes.at[:, at], ins.at[i])

    def store(i):
        at = pl.ds(i * owners * block, owners * block)
        return pltpu.make_async_copy(fresh.at[at], out_hbm.at[at], outs.at[i])

    for i in range(dp_n // owners):
        load(i).start()
    take = pltpu.make_async_copy(cost_in, cost, row.at[0])
    give = pltpu.make_async_copy(cost, cost_out, row.at[1])
    take.start()

    def owner(o, carry):
        for p in range(pairs):
            for s in range(2):
                cols = slice(s * side_w + p * part, s * side_w + (p + 1) * part)
                for g in range(half // size):
                    packed = codes[p, o, s * half + g * size : s * half + (g + 1) * size]
                    bits = ((packed[:8] >> 16) & 1).astype(jnp.float32)
                    word = jnp.sum(bits * weight, axis=1, keepdims=True) - FINE_BIAS
                    scale = jnp.exp2(word * (1.0 / FINE)) * (1.0 / STEPS)
                    scale = jnp.broadcast_to(scale[0:1], (1, part))
                    at = pl.multiple_of(o * block, block) + g * size
                    fresh[pl.ds(at, size), cols] = (packed >> 16).astype(jnp.float32) * scale
                    low = ((packed << 16) >> 16).astype(jnp.float32)
                    fresh[pl.ds(at + half, size), cols] = low * scale
        return carry

    for i in range(dp_n // owners):
        load(i).wait()
        lax.fori_loop(i * owners, (i + 1) * owners, owner, 0)
        store(i).start()
    take.wait()
    give.start()
    for i in range(dp_n // owners):
        store(i).wait()
    give.wait()


def shards(points, centroids, assign, keep_mask):
    rows, width = points.shape
    shard_rows = centroids.shape[0]
    z_n = lax.axis_size("z")
    dp_n = z_n * PLANE
    block = shard_rows // dp_n
    kept = z_n * block
    part = LANES
    side_w = width // 2
    pairs = side_w // part
    vmem = pl.BlockSpec(memory_space=pltpu.VMEM)
    hbm = pl.BlockSpec(memory_space=pltpu.HBM)
    dma = pltpu.SemaphoreType.DMA
    by_pair = dma((2, pairs))
    by_z = dma((pairs, z_n))
    halves = dma((pairs, 2))
    by_step = dma((pairs, (z_n - 1).bit_length(), 2))
    by_half = dma((pairs, z_n, 2))
    by_quarter = dma((pairs, z_n, 4))
    codes, cost = pl.pallas_call(
        functools.partial(update_kernel, z_n, pairs),
        out_shape=(
            jax.ShapeDtypeStruct((pairs, dp_n, block, part), jnp.int32),
            jax.ShapeDtypeStruct((1, rows), jnp.float32),
        ),
        in_specs=[hbm] * 4,
        out_specs=(hbm, vmem),
        scratch_shapes=[
            pltpu.VMEM((pairs, dp_n, block, part), jnp.int32),
            pltpu.VMEM((2 * rows, width), points.dtype),
            pltpu.VMEM((shard_rows, width), centroids.dtype),
            pltpu.VMEM((2, 1, rows), jnp.int32),
            pltpu.VMEM((block, width), centroids.dtype),
            pltpu.VMEM((6, 1, rows), jnp.int32),
            pltpu.VMEM((2, 1, 2 * rows), jnp.int32),
            pltpu.VMEM((4, 2 * kept, 2 * rows), jnp.bfloat16),
            pltpu.VMEM((2, 2 * rows, side_w), points.dtype),
            pltpu.VMEM((2, 2 * kept, side_w), jnp.float32),
            pltpu.VMEM((2 * kept, LANES), jnp.float32),
            pltpu.VMEM((2, pairs, kept // 2, part), jnp.int32),
            pltpu.VMEM((2, pairs, kept // 2, part), jnp.int32),
            pltpu.VMEM((pairs, z_n, block, part), jnp.int32),
            pltpu.VMEM((pairs, z_n, block, part), jnp.int32),
            pltpu.VMEM((1, 2 * rows), jnp.float32),
            pltpu.VMEM((1, rows), jnp.float32),
            dma((5,)), dma((5,)), dma((5,)), dma, dma,
            by_pair, by_pair, by_pair, by_pair, by_pair, by_pair,
            by_step, by_step, by_z, by_z, by_z, by_z, by_z, by_z, by_z, by_z, by_z, by_z, by_z,
            halves, halves, by_quarter, by_quarter, by_half, by_half, by_half, by_half,
            dma, dma,
        ],
        compiler_params=pltpu.CompilerParams(
            collective_id=0, has_side_effects=True, vmem_limit_bytes=56 * 1024 * 1024
        ),
        cost_estimate=pl.CostEstimate(
            flops=0, bytes_accessed=200 * 1024 * 1024, transcendentals=0
        ),
        name="update",
    )(points, centroids, assign.reshape(1, rows), keep_mask.reshape(1, rows))
    new_centroids, cost = pl.pallas_call(
        decode_kernel,
        in_specs=[hbm, hbm],
        out_specs=(hbm, hbm),
        out_shape=(
            jax.ShapeDtypeStruct((shard_rows, width), jnp.float32),
            jax.ShapeDtypeStruct((1, rows), jnp.float32),
        ),
        scratch_shapes=[
            pltpu.VMEM((pairs, dp_n, block, part), jnp.int32),
            pltpu.VMEM((shard_rows, width), jnp.float32),
            pltpu.VMEM((1, rows), jnp.float32),
            dma((dp_n,)), dma((dp_n,)), dma((2,)),
        ],
        compiler_params=pltpu.CompilerParams(vmem_limit_bytes=56 * 1024 * 1024),
        name="decode",
    )(codes, cost)
    return new_centroids, cost.reshape(rows)


def solution(mesh):
    dp, mp = mesh.shape["dp"], mesh.shape["mp"]
    grid = Mesh(mesh.devices.reshape(dp // PLANE, PLANE, mp), ("z", "q", "mp"))
    rows = ("z", "q", "mp")
    in_specs = (P(rows, None), P("mp", None), P(rows), P(rows))
    out_specs = (P("mp", None), P(rows))
    return jax.shard_map(shards, mesh=grid, in_specs=in_specs, out_specs=out_specs, check_vma=False)
```

```python
import functools

import jax
import jax.numpy as jnp
from jax import lax
from jax.experimental import pallas as pl
from jax.experimental.pallas import tpu as pltpu
from jax.sharding import Mesh
from jax.sharding import PartitionSpec as P

STEPS = 32000.0
TINY = 2.0**-100
BIAS = 128
EXP = 8
WORD = 32
GROUP = 16
FINE = 8.0
FINE_BIAS = 1024
FINE_BITS = 12
PLANE = 4
LATE = 2
LANES = 128
CTILE = 256
MESH = pl.DeviceIdType.MESH


def remote(src, dst, send, recv, device):
    return pltpu.make_async_remote_copy(
        src_ref=src, dst_ref=dst, send_sem=send, recv_sem=recv, device_id=device, device_id_type=MESH
    )


def repeat(n, body):
    if n <= 4:
        for t in range(n):
            body(t)
    else:
        lax.fori_loop(0, n, lambda t, carry: (body(t), carry)[1], 0)


def span(t, size, start=0):
    at = start + t * size
    return pl.ds(at if isinstance(at, int) else pl.multiple_of(at, size), size)


def power_of(top):
    return jnp.ceil(jnp.log2(jnp.maximum(top, TINY)))


def quantize(v, power):
    return jnp.floor(v * (jnp.exp2(-power) * STEPS) + 0.5).astype(jnp.int32)


def embed(code, power, count=None):
    lane = lax.broadcasted_iota(jnp.int32, code.shape, 1)
    bit = lax.shift_right_logical(jnp.broadcast_to(power, code.shape), jnp.minimum(lane, 31)) & 1
    used = EXP
    if count is not None:
        at = jnp.clip(lane - EXP, 0, 31)
        bit = jnp.where(lane < EXP, bit, lax.shift_right_logical(jnp.broadcast_to(count, code.shape), at) & 1)
        used = WORD
    return (code & jnp.where(lane < used, -2, -1)) | bit


def pack(code):
    half = code.shape[0] // 2
    return (code[:half] << 16) | (code[half:] & 0xFFFF)


def unpack(packed):
    return jnp.concatenate([packed >> 16, (packed << 16) >> 16], axis=0)


def bits_word(code, lo, hi):
    lane = lax.broadcasted_iota(jnp.int32, (1, LANES), 1)
    weight = jnp.where((lane >= lo) & (lane < hi), 1 << jnp.clip(lane - lo, 0, hi - lo), 0)
    bits = (code[:, :LANES] & 1).astype(jnp.float32)
    return jnp.sum(bits * weight.astype(jnp.float32), axis=1, keepdims=True)


def scale_of(code):
    return jnp.exp2(bits_word(code, 0, EXP) - BIAS) * (1.0 / STEPS)


def count_of(code):
    return bits_word(code, EXP, WORD)


def encode(v, count=None):
    power = power_of(jnp.max(jnp.abs(v), axis=1, keepdims=True))
    if count is not None:
        count = count.astype(jnp.int32)
    return pack(embed(quantize(v, power), power.astype(jnp.int32) + BIAS, count))


def decode(packed):
    code = unpack(packed)
    return code.astype(jnp.float32) * scale_of(code)


def group_of(half):
    return min(GROUP, half)


def publish_code(v):
    half = v.shape[0] // 2
    size = group_of(half)
    lane = lax.broadcasted_iota(jnp.int32, (size, LANES), 1)
    out = []
    for g in range(half // size):
        hi, lo = v[g * size : (g + 1) * size], v[half + g * size : half + (g + 1) * size]
        top = jnp.max(jnp.maximum(jnp.abs(hi), jnp.abs(lo)), axis=0, keepdims=True)
        top = jnp.maximum(jnp.max(top, axis=1, keepdims=True), TINY)
        word = jnp.ceil(jnp.log2(top) * FINE)
        factor = jnp.exp2(word * (-1.0 / FINE)) * STEPS
        codes = [jnp.floor(part * factor + 0.5).astype(jnp.int32) for part in (hi, lo)]
        bit = lax.shift_right_logical(
            jnp.broadcast_to(word.astype(jnp.int32) + FINE_BIAS, (size, LANES)), jnp.minimum(lane, 31)
        ) & 1
        first = (codes[0] & jnp.where(lane < FINE_BITS, -2, -1)) | jnp.where(lane < FINE_BITS, bit, 0)
        out.append((first << 16) | (codes[1] & 0xFFFF))
    return jnp.concatenate(out, axis=0)


TUNED = {
    (4, 4, 8): (
        0, 15, 17, 21, 31, 2, 13, 16, 26, 33, 32, 40, 34, 44, 55, 69, 92, 65, 100, 125,
        66, 78, 131, 81, 90, 142, 76, 93, 111, 88, 120, 127, 80, 96, 137, 1, 18, 22, 35, 37,
        3, 20, 23, 39, 41, 38, 49, 42, 54, 61, 71, 118, 72, 112, 135, 74, 102, 134, 83, 97,
        130, 79, 94, 117, 98, 106, 129, 95, 114, 144, 25, 46, 50, 57, 60, 30, 53, 56, 63, 67,
        64, 75, 68, 77, 86, 101, 136, 109, 132, 105, 126, 113, 139, 119, 143, 121, 145, 124, 146, 4,
        24, 29, 43, 45, 5, 28, 36, 48, 51, 47, 59, 52, 58, 73, 82, 104, 91, 115, 87, 128,
        103, 141, 108, 122, 107, 133, 116, 140, 6, 7, 12, 14, 19, 8, 9, 10, 11, 27, 62, 70,
        84, 85, 89, 99, 110, 123, 138,
    ),
}


def schedule(z_n, pairs, tiles):
    times = {}
    for p in range(pairs):
        at = 9.0 + 3.0 * p
        for s in range(2):
            times["P", p, s] = 0.01 * p if p < pairs - 1 else 9.1
            times["A", p, s] = at + 0.01 * s
            times["B1", p, s] = at + 0.1 + 0.01 * s
            times["B2", p, s] = at + 0.5 + 0.01 * s
            times["C", p, s] = at + 8.0 + 0.01 * s
        steps = (z_n - 1).bit_length()
        for s in range(2):
            times["Z", p, s] = at + 8.1 + 0.01 * s
            for b in range(1, steps):
                times["H", p, b, s] = at + 8.0 + 5.5 * b + 0.01 * s
        done = max(26.0 + 4.0 * p, at + 8.0 + 5.5 * steps)
        times["D", p] = done
        if p >= pairs - LATE:
            times["F", p] = done + 3.2
        for k in range(z_n):
            for d in range(2 if k else 1):
                if k:
                    times["E", p, k, d] = done + 3.5 * k
                if p < pairs - LATE:
                    times["R", p, k, d] = done + 3.5 * k + 3.2
                times["S", p, k, d] = done + 3.5 * k + 6.8
    times["mate",] = 0.005
    for s in range(2):
        times["hitO", s] = 2.0 + 0.1 * s
        times["hitN", s] = 4.6 + 0.1 * s
        times["own", s, 1] = 4.0 + 0.1 * s
        times["own", s, 0] = 4.3 + 0.1 * s
    for i in range(tiles):
        times["L", i] = 26.5 + 1.5 * i
    times["X",] = 27.0 + 1.5 * tiles
    times["Y",] = 33.0 + 1.5 * tiles
    tuned = TUNED.get((z_n, pairs, tiles))
    if tuned is not None:
        times = dict(zip(times, tuned, strict=True))
    return sorted(times, key=lambda task: times[task])


def update_kernel(
    z_n, pairs, p_hbm, c_hbm, assign_hbm, keep_hbm, code_hbm, cost_ref,
    out_ref, p2, cents, ak, prior, idv, slot, hit, pn, acc, cnt, asend, arecv, zsend, zrecv, low, lowr,
    loc, ids_s, ids_r, mt_s, mt_r, ps, pr, fs, fr, as_, ar, zs, zr,
    grs, grr, gls, glr, xs, xr, ys, yr, ds_, dr, outs, f1s, f1r, f2s, f2r, hrs, hrr, hls, hlr, lo_s, lo_r,
):
    z, q, m = lax.axis_index("z"), lax.axis_index("q"), lax.axis_index("mp")
    nx = q + 1 - 2 * lax.rem(q, 2)
    ny = lax.rem(q + 2, PLANE)
    other = 1 - m
    rows, width = p_hbm.shape
    shard_rows = c_hbm.shape[0]
    block = prior.shape[0]
    both = 2 * rows
    kept = z_n * block
    side_w = width // 2
    part = side_w // pairs
    last = z_n - 1
    bits = last.bit_length()
    up, down = lax.rem(z + 1, z_n), lax.rem(z + last, z_n)
    own = z * PLANE + q
    near, far = (nx, ny), (ny, nx)

    load_p = pltpu.make_async_copy(p_hbm, p2.at[pl.ds(0, rows)], loc.at[0])
    load_prior = pltpu.make_async_copy(
        c_hbm.at[pl.ds(pl.multiple_of(own * block, block), block)], prior, loc.at[1]
    )
    load_c = pltpu.make_async_copy(c_hbm, cents, loc.at[2])
    load_a = pltpu.make_async_copy(assign_hbm, ak.at[0], loc.at[3])
    load_k = pltpu.make_async_copy(keep_hbm, ak.at[1], loc.at[4])
    for copy in (load_a, load_k, load_p):
        copy.start()

    barrier = pltpu.get_barrier_semaphore()
    peers = [(z, q, other), (z, nx, m), (z, nx, other), (z, ny, m), (z, ny, other)]
    greet = peers + [(lax.rem(z + k, z_n), q, m) for k in range(1, z_n)]
    for peer in greet:
        pl.semaphore_signal(barrier, inc=1, device_id=peer, device_id_type=MESH)
    load_a.wait()
    load_k.wait()
    idv[0] = jnp.where(ak[1] > 0, ak[0], -1)
    load_c.start()
    load_prior.start()
    pl.semaphore_wait(barrier, len(greet))

    def pts_copy(s, p):
        cols = pl.ds(s * side_w + p * part, part)
        return remote(
            p2.at[pl.ds(0, rows), cols], pn.at[s, pl.ds(0, rows), pl.ds(p * part, part)], ps.at[s, p], pr.at[s, p],
            (z, near[s], m),
        )

    def fwd_copy(s, p):
        return remote(
            pn.at[s, pl.ds(0, rows), pl.ds(p * part, part)], pn.at[s, pl.ds(rows, rows), pl.ds(p * part, part)], fs.at[s, p], fr.at[s, p],
            (z, q, other),
        )

    def a_copy(s, p):
        return remote(asend.at[s, p], arecv.at[s, p], as_.at[s, p], ar.at[s, p], (z, far[s], m))

    def side_of(s):
        return slice(s * (block // 2), (s + 1) * (block // 2))

    def z_copy(p, b, s):
        n = z_n >> (b + 1)
        at = pl.ds(z_n - 2 * n, n)
        bit = lax.rem(lax.div(z, 1 << b), 2)
        to = z + (1 << b) * (1 - 2 * bit)
        return remote(
            zsend.at[p, at, side_of(s)], zrecv.at[p, at, side_of(s)], zs.at[p, b, s], zr.at[p, b, s], (to, q, m)
        )

    id_copies = [
        remote(idv.at[0], idv.at[k + 1], ids_s.at[k], ids_r.at[k], peer) for k, peer in enumerate(peers)
    ]
    mate_copy = remote(p2.at[pl.ds(0, rows)], p2.at[pl.ds(rows, rows)], mt_s, mt_r, (z, q, other))

    load_p.wait()
    for copy in id_copies:
        copy.start()

    def slots_of(s, a, b):
        ids = jnp.concatenate([idv[a], idv[b]], axis=1) - m * shard_rows
        inside = (ids >= 0) & (ids < shard_rows)
        ids = jnp.where(inside, ids, 0)
        owner = lax.rem(lax.div(ids, block), PLANE)
        at = lax.div(ids, block * PLANE) * block + lax.rem(ids, block)
        found = jnp.where(owner == q, at, jnp.where(owner == far[s], at + kept, -1))
        return jnp.where(inside, found, -1)

    def fill_hits(s, first):
        group = s if first else 2 + s
        slot[s] = slots_of(s, *((0, 1) if first else ((2, 3), (4, 5))[s]))

        def tile(t, carry):
            base = pl.multiple_of(t * LANES, LANES)
            row = lax.broadcasted_iota(jnp.int32, (LANES, both), 0) + base
            hit[group, pl.ds(base, LANES), :] = jnp.where(row == slot[s], 1.0, 0.0).astype(jnp.bfloat16)
            return carry

        lax.fori_loop(0, 2 * kept // LANES, tile, 0)

    ones = jnp.ones((both, LANES), jnp.bfloat16)

    def own_dot(s, half):
        at = pl.ds(half * kept, kept)
        acc[s, at, :] = jnp.dot(
            hit[s, at, :], p2[:, s * side_w : (s + 1) * side_w], preferred_element_type=jnp.float32
        )
        if s == 0:
            cnt[at, :] = jnp.dot(hit[s, at, :], ones, preferred_element_type=jnp.float32)

    def near_dot(s, p, half):
        at, cols = pl.ds(half * kept, kept), pl.ds(p * part, part)
        points = pn[s, :, p * part : (p + 1) * part]
        if s == 0 and p == 0:
            points = jnp.concatenate([points, ones], axis=1)
        more = jnp.dot(hit[2 + s, at, :], points, preferred_element_type=jnp.float32)
        acc[s, at, cols] += more[:, :part]
        if s == 0 and p == 0:
            cnt[at, :] += more[:, part:]

    def rows_of(t):
        return span(t, block)

    def half_rows_of(t):
        return span(t, block // 2)

    def step_a(p, s):
        pts_copy(s, p).wait_recv()
        fwd_copy(s, p).start()

    def step_b(p, s):
        fwd_copy(s, p).wait_recv()
        near_dot(s, p, 1)

        def tile(t):
            at = span(t, block, kept)
            count = cnt[at, 0:1] if s == 0 and p == 0 else None
            asend[s, p, half_rows_of(t), :] = encode(acc[s, at, p * part : (p + 1) * part], count)

        repeat(z_n, tile)
        a_copy(s, p).start()

    def step_b2(p, s):
        near_dot(s, p, 0)

    def target(b, j, mine):
        bit = lax.rem(lax.div(z, 1 << b), 2)
        return j * (2 << b) + lax.rem(z, 1 << b) + (bit if mine else 1 - bit) * (1 << b)

    def z_send(p, b, s):
        n = z_n >> (b + 1)

        def tile(j):
            at = rows_of(target(b, j, False))
            count = cnt[at, 0:1] if s == 0 and p == 0 else None
            zsend[p, z_n - 2 * n + j, side_of(s), :] = encode(acc[s, at, p * part : (p + 1) * part], count)

        repeat(n, tile)
        z_copy(p, b, s).start()

    def gain(s, p, at, packed):
        acc[s, at, p * part : (p + 1) * part] += decode(packed)
        if s == 0 and p == 0:
            cnt[at, :] = jnp.broadcast_to(cnt[at, 0:1] + count_of(unpack(packed)), (block, LANES))

    def step_c(p, s):
        a_copy(s, p).wait_recv()

        def tile(t):
            gain(s, p, rows_of(t), arecv[s, p, half_rows_of(t), :])

        repeat(z_n, tile)

    def z_gain(p, b, s):
        n = z_n >> (b + 1)
        z_copy(p, b, s).wait_recv()

        def tile(j):
            gain(s, p, rows_of(target(b, j, True)), zrecv[p, z_n - 2 * n + j, side_of(s), :])

        repeat(n, tile)

    def step_h(p, b, s):
        z_gain(p, b - 1, s)
        z_send(p, b, s)

    def xcopy(p, n, to_q):
        at = out_ref.at[p, n * PLANE + to_q]
        return remote(at, at, xs.at[p, n], xr.at[p, n], (z, nx, m))

    def ycopy(p, n, to_q):
        at = out_ref.at[p, n * PLANE + to_q]
        return remote(at, at, ys.at[p, n], yr.at[p, n], (z, ny, m))

    def dcopy(p, n, by_x):
        at = out_ref.at[p, n * PLANE + (nx if by_x else ny)]
        return remote(at, at, ds_.at[p, n], dr.at[p, n], (z, ny if by_x else nx, m))

    def gright(p, n):
        at = out_ref.at[p, n * PLANE + q]
        return remote(at, at, grs.at[p, n], grr.at[p, n], (up, q, m))

    def gleft(p, n):
        at = out_ref.at[p, n * PLANE + q]
        return remote(at, at, gls.at[p, n], glr.at[p, n], (down, q, m))

    def late(p):
        return p >= pairs - LATE

    def first_copy(p, s):
        at = out_ref.at[p, own, side_of(s)]
        return remote(at, at, f1s.at[p, s], f1r.at[p, s], (z, near[s], m))

    def second_copy(p, n, s, j):
        at = out_ref.at[p, n * PLANE + (near[s] if j else q), side_of(s)]
        i = 2 * s + j
        return remote(at, at, f2s.at[p, n, i], f2r.at[p, n, i], (z, far[s], m))

    def hright(p, n, s):
        at = out_ref.at[p, n * PLANE + near[s], side_of(s)]
        return remote(at, at, hrs.at[p, n, s], hrr.at[p, n, s], (up, q, m))

    def hleft(p, n, s):
        at = out_ref.at[p, n * PLANE + near[s], side_of(s)]
        return remote(at, at, hls.at[p, n, s], hlr.at[p, n, s], (down, q, m))

    def step_f(p):
        for s in range(2):
            first_copy(p, s).wait_recv()

        @pl.when(z < last)
        def _():
            for s in range(2):
                hright(p, z, s).start()

        @pl.when(z > 0)
        def _():
            for s in range(2):
                hleft(p, z, s).start()

        for s in range(2):
            second_copy(p, z, s, 1).start()

    def step_d(p):
        mine = rows_of(z)
        for s in range(2):
            z_gain(p, bits - 1, s)
        if p == 0:
            load_prior.wait()
        count = cnt[mine, 0:1]
        fresh = []
        for s in range(2):
            lo = s * side_w + p * part
            total = acc[s, mine, p * part : (p + 1) * part]
            fallback = prior[:, lo : lo + part].astype(jnp.float32)
            fresh.append(jnp.where(count > 0.5, total / jnp.maximum(count, 1.0), fallback))
        for s in range(2):
            out_ref[p, own, side_of(s)] = publish_code(fresh[s])

        @pl.when(z < last)
        def _():
            gright(p, z).start()

        @pl.when(z > 0)
        def _():
            gleft(p, z).start()

        if late(p):
            for s in range(2):
                first_copy(p, s).start()
            for s in range(2):
                second_copy(p, z, s, 0).start()
            return

        xcopy(p, z, q).start()
        ycopy(p, z, q).start()

    def relay(p, n, by_x):
        if by_x:
            xcopy(p, n, nx).wait_recv()
        else:
            ycopy(p, n, ny).wait_recv()
        dcopy(p, n, by_x).start()

    def settle(p, n, by_x):
        if late(p):
            for s in range(2):
                for j in range(2):
                    second_copy(p, n, s, j).wait_recv()
            put(p, n).start()
            return
        if by_x:
            ycopy(p, n, ny).wait_recv()
        else:
            xcopy(p, n, nx).wait_recv()
        dcopy(p, n, by_x).wait_recv()

        put(p, n).start()

    def put(p, n):
        at = pl.ds(n * PLANE, PLANE)
        return pltpu.make_async_copy(out_ref.at[p, at], code_hbm.at[p, at], outs.at[p, n])

    def each(p, k, d, action):
        if k == 0:
            action(p, z, p % 2 == 0)
            return

        @pl.when((z >= k) if d == 0 else (z + k <= last))
        def _():
            action(p, z - k if d == 0 else z + k, (k + p) % 2 == d)

    def spread(p, k, d):
        @pl.when((z >= k) if d == 0 else (z + k <= last))
        def _():
            n, hop = (z - k, gright) if d == 0 else (z + k, gleft)
            hop(p, n).wait_recv()

            @pl.when((z < last) if d == 0 else (z > 0))
            def _():
                hop(p, n).start()

            if not late(p):
                xcopy(p, n, q).start()
                ycopy(p, n, q).start()
                return

            for s in range(2):
                second_copy(p, n, s, 0).start()
            hops = hright if d == 0 else hleft
            for s in range(2):
                hops(p, n, s).wait_recv()

            @pl.when((z < last) if d == 0 else (z > 0))
            def _():
                for s in range(2):
                    hops(p, n, s).start()

            for s in range(2):
                second_copy(p, n, s, 1).start()

    met = []

    def meet():
        if not met:
            met.append(True)
            mate_copy.wait_recv()

    seen = []

    def lowest():
        i = len(seen)
        seen.append(i)
        meet()
        if i == 0:
            load_c.wait()

        def tile(t, best):
            tile_ref = cents[pl.ds(pl.multiple_of(t * CTILE, CTILE), CTILE), :]
            wide = tile_ref.astype(jnp.float32)
            sq = jnp.sum(wide * wide, axis=1, keepdims=True)
            inner = lax.dot_general(
                tile_ref, p2[...], (((1,), (1,)), ((), ())), preferred_element_type=jnp.float32
            )
            return jnp.minimum(best, jnp.min(sq - 2.0 * inner, axis=0, keepdims=True))

        start = jnp.full((1, both), jnp.inf, jnp.float32) if i == 0 else low[...]
        low[...] = lax.fori_loop(i, i + 1, tile, start)

    low_copy = remote(low.at[:, pl.ds(rows, rows)], lowr, lo_s, lo_r, (z, q, other))

    def finish_cost():
        low_copy.wait_recv()
        wide = p2[pl.ds(0, rows), :].astype(jnp.float32)
        sq = jnp.sum(wide * wide, axis=1, keepdims=True)
        flat = jnp.broadcast_to(sq, (rows, LANES)).T[0:1, :]
        cost_ref[...] = (flat + jnp.minimum(low[:, :rows], lowr[...])) / width

    greeted = []

    def hits(s, first):
        if not greeted:
            greeted.append(True)
            for copy in id_copies:
                copy.wait_recv()
        fill_hits(s, first)

    def own_part(s, half):
        meet()
        own_dot(s, half)

    actions = {
        "P": lambda p, s: pts_copy(s, p).start(), "mate": mate_copy.start,
        "hitO": lambda s: hits(s, True), "hitN": lambda s: hits(s, False), "own": own_part,
        "A": step_a, "B1": step_b, "B2": step_b2, "C": step_c, "Z": lambda p, s: z_send(p, 0, s), "H": step_h,
        "D": step_d, "F": step_f, "E": spread, "R": lambda p, k, d: each(p, k, d, relay),
        "S": lambda p, k, d: each(p, k, d, settle), "L": lambda i: lowest(),
        "X": low_copy.start, "Y": finish_cost,
    }
    for task in schedule(z_n, pairs, shard_rows // CTILE):
        actions[task[0]](*task[1:])

    for copy in id_copies + [mate_copy, low_copy]:
        copy.wait_send()
    for p in range(pairs):
        for s in range(2):
            if late(p):
                first_copy(p, s).wait_send()
            pts_copy(s, p).wait_send()
            fwd_copy(s, p).wait_send()
            a_copy(s, p).wait_send()
        for t in range(z_n):
            if t < bits:
                for s in range(2):
                    z_copy(p, t, s).wait_send()

            @pl.when((z >= t) & (z < last))
            def _(p=p, t=t):
                gright(p, t).wait_send()
                if late(p):
                    for s in range(2):
                        hright(p, t, s).wait_send()

            @pl.when((z <= t) & (z > 0))
            def _(p=p, t=t):
                gleft(p, t).wait_send()
                if late(p):
                    for s in range(2):
                        hleft(p, t, s).wait_send()

            put(p, t).wait()
            if late(p):
                for s in range(2):
                    for j in range(2):
                        second_copy(p, t, s, j).wait_send()
                continue
            xcopy(p, t, q).wait_send()
            ycopy(p, t, q).wait_send()
            dcopy(p, t, True).wait_send()


def decode_kernel(in_hbm, cost_in, out_hbm, cost_out, codes, fresh, cost, ins, outs, row):
    pairs, dp_n, block, part = codes.shape
    half = block // 2
    size = group_of(half)
    side_w = fresh.shape[1] // 2
    lane = lax.broadcasted_iota(jnp.int32, (1, LANES), 1)
    weight = jnp.where(lane < FINE_BITS, 1 << jnp.minimum(lane, FINE_BITS), 0).astype(jnp.float32)
    owners = max(1, min(dp_n, 256 // block))

    def load(i):
        at = pl.ds(i * owners, owners)
        return pltpu.make_async_copy(in_hbm.at[:, at], codes.at[:, at], ins.at[i])

    def store(i):
        at = pl.ds(i * owners * block, owners * block)
        return pltpu.make_async_copy(fresh.at[at], out_hbm.at[at], outs.at[i])

    for i in range(dp_n // owners):
        load(i).start()
    take = pltpu.make_async_copy(cost_in, cost, row.at[0])
    give = pltpu.make_async_copy(cost, cost_out, row.at[1])
    take.start()

    def owner(o, carry):
        for p in range(pairs):
            for s in range(2):
                cols = slice(s * side_w + p * part, s * side_w + (p + 1) * part)
                for g in range(half // size):
                    packed = codes[p, o, s * half + g * size : s * half + (g + 1) * size]
                    bits = ((packed[:8] >> 16) & 1).astype(jnp.float32)
                    word = jnp.sum(bits * weight, axis=1, keepdims=True) - FINE_BIAS
                    scale = jnp.exp2(word * (1.0 / FINE)) * (1.0 / STEPS)
                    scale = jnp.broadcast_to(scale[0:1], (1, part))
                    at = pl.multiple_of(o * block, block) + g * size
                    fresh[pl.ds(at, size), cols] = (packed >> 16).astype(jnp.float32) * scale
                    low = ((packed << 16) >> 16).astype(jnp.float32)
                    fresh[pl.ds(at + half, size), cols] = low * scale
        return carry

    for i in range(dp_n // owners):
        load(i).wait()
        lax.fori_loop(i * owners, (i + 1) * owners, owner, 0)
        store(i).start()
    take.wait()
    give.start()
    for i in range(dp_n // owners):
        store(i).wait()
    give.wait()


def shards(points, centroids, assign, keep_mask):
    rows, width = points.shape
    shard_rows = centroids.shape[0]
    z_n = lax.axis_size("z")
    dp_n = z_n * PLANE
    block = shard_rows // dp_n
    kept = z_n * block
    part = LANES
    side_w = width // 2
    pairs = side_w // part
    vmem = pl.BlockSpec(memory_space=pltpu.VMEM)
    hbm = pl.BlockSpec(memory_space=pltpu.HBM)
    dma = pltpu.SemaphoreType.DMA
    by_pair = dma((2, pairs))
    by_z = dma((pairs, z_n))
    halves = dma((pairs, 2))
    by_step = dma((pairs, (z_n - 1).bit_length(), 2))
    by_half = dma((pairs, z_n, 2))
    by_quarter = dma((pairs, z_n, 4))
    codes, cost = pl.pallas_call(
        functools.partial(update_kernel, z_n, pairs),
        out_shape=(
            jax.ShapeDtypeStruct((pairs, dp_n, block, part), jnp.int32),
            jax.ShapeDtypeStruct((1, rows), jnp.float32),
        ),
        in_specs=[hbm] * 4,
        out_specs=(hbm, vmem),
        scratch_shapes=[
            pltpu.VMEM((pairs, dp_n, block, part), jnp.int32),
            pltpu.VMEM((2 * rows, width), points.dtype),
            pltpu.VMEM((shard_rows, width), centroids.dtype),
            pltpu.VMEM((2, 1, rows), jnp.int32),
            pltpu.VMEM((block, width), centroids.dtype),
            pltpu.VMEM((6, 1, rows), jnp.int32),
            pltpu.VMEM((2, 1, 2 * rows), jnp.int32),
            pltpu.VMEM((4, 2 * kept, 2 * rows), jnp.bfloat16),
            pltpu.VMEM((2, 2 * rows, side_w), points.dtype),
            pltpu.VMEM((2, 2 * kept, side_w), jnp.float32),
            pltpu.VMEM((2 * kept, LANES), jnp.float32),
            pltpu.VMEM((2, pairs, kept // 2, part), jnp.int32),
            pltpu.VMEM((2, pairs, kept // 2, part), jnp.int32),
            pltpu.VMEM((pairs, z_n, block, part), jnp.int32),
            pltpu.VMEM((pairs, z_n, block, part), jnp.int32),
            pltpu.VMEM((1, 2 * rows), jnp.float32),
            pltpu.VMEM((1, rows), jnp.float32),
            dma((5,)), dma((5,)), dma((5,)), dma, dma,
            by_pair, by_pair, by_pair, by_pair, by_pair, by_pair,
            by_step, by_step, by_z, by_z, by_z, by_z, by_z, by_z, by_z, by_z, by_z, by_z, by_z,
            halves, halves, by_quarter, by_quarter, by_half, by_half, by_half, by_half,
            dma, dma,
        ],
        compiler_params=pltpu.CompilerParams(
            collective_id=0, has_side_effects=True, vmem_limit_bytes=56 * 1024 * 1024
        ),
        cost_estimate=pl.CostEstimate(
            flops=0, bytes_accessed=200 * 1024 * 1024, transcendentals=0
        ),
        name="update",
    )(points, centroids, assign.reshape(1, rows), keep_mask.reshape(1, rows))
    new_centroids, cost = pl.pallas_call(
        decode_kernel,
        in_specs=[hbm, hbm],
        out_specs=(hbm, hbm),
        out_shape=(
            jax.ShapeDtypeStruct((shard_rows, width), jnp.float32),
            jax.ShapeDtypeStruct((1, rows), jnp.float32),
        ),
        scratch_shapes=[
            pltpu.VMEM((pairs, dp_n, block, part), jnp.int32),
            pltpu.VMEM((shard_rows, width), jnp.float32),
            pltpu.VMEM((1, rows), jnp.float32),
            dma((dp_n,)), dma((dp_n,)), dma((2,)),
        ],
        compiler_params=pltpu.CompilerParams(vmem_limit_bytes=56 * 1024 * 1024),
        name="decode",
    )(codes, cost)
    return new_centroids, cost.reshape(rows)


def solution(mesh):
    dp, mp = mesh.shape["dp"], mesh.shape["mp"]
    grid = Mesh(mesh.devices.reshape(dp // PLANE, PLANE, mp), ("z", "q", "mp"))
    rows = ("z", "q", "mp")
    in_specs = (P(rows, None), P("mp", None), P(rows), P(rows))
    out_specs = (P("mp", None), P(rows))
    return jax.shard_map(shards, mesh=grid, in_specs=in_specs, out_specs=out_specs, check_vma=False)
```

```python
import functools

import jax
import jax.numpy as jnp
from jax import lax
from jax.experimental import pallas as pl
from jax.experimental.pallas import tpu as pltpu
from jax.sharding import Mesh
from jax.sharding import PartitionSpec as P

STEPS = 32000.0
TINY = 2.0**-100
BIAS = 128
EXP = 8
WORD = 32
GROUP = 16
FINE = 8.0
FINE_BIAS = 1024
FINE_BITS = 12
PLANE = 4
LATE = 2
LANES = 128
CTILE = 256
MESH = pl.DeviceIdType.MESH


def remote(src, dst, send, recv, device):
    return pltpu.make_async_remote_copy(
        src_ref=src, dst_ref=dst, send_sem=send, recv_sem=recv, device_id=device, device_id_type=MESH
    )


def repeat(n, body):
    if n <= 4:
        for t in range(n):
            body(t)
    else:
        lax.fori_loop(0, n, lambda t, carry: (body(t), carry)[1], 0)


def span(t, size, start=0):
    at = start + t * size
    return pl.ds(at if isinstance(at, int) else pl.multiple_of(at, size), size)


def power_of(top):
    return jnp.ceil(jnp.log2(jnp.maximum(top, TINY)))


def quantize(v, power):
    return jnp.floor(v * (jnp.exp2(-power) * STEPS) + 0.5).astype(jnp.int32)


def embed(code, power, count=None):
    lane = lax.broadcasted_iota(jnp.int32, code.shape, 1)
    bit = lax.shift_right_logical(jnp.broadcast_to(power, code.shape), jnp.minimum(lane, 31)) & 1
    used = EXP
    if count is not None:
        at = jnp.clip(lane - EXP, 0, 31)
        bit = jnp.where(lane < EXP, bit, lax.shift_right_logical(jnp.broadcast_to(count, code.shape), at) & 1)
        used = WORD
    return (code & jnp.where(lane < used, -2, -1)) | bit


def pack(code):
    half = code.shape[0] // 2
    return (code[:half] << 16) | (code[half:] & 0xFFFF)


def unpack(packed):
    return jnp.concatenate([packed >> 16, (packed << 16) >> 16], axis=0)


def bits_word(code, lo, hi):
    lane = lax.broadcasted_iota(jnp.int32, (1, LANES), 1)
    weight = jnp.where((lane >= lo) & (lane < hi), 1 << jnp.clip(lane - lo, 0, hi - lo), 0)
    bits = (code[:, :LANES] & 1).astype(jnp.float32)
    return jnp.sum(bits * weight.astype(jnp.float32), axis=1, keepdims=True)


def scale_of(code):
    return jnp.exp2(bits_word(code, 0, EXP) - BIAS) * (1.0 / STEPS)


def count_of(code):
    return bits_word(code, EXP, WORD)


def encode(v, count=None):
    power = power_of(jnp.max(jnp.abs(v), axis=1, keepdims=True))
    if count is not None:
        count = count.astype(jnp.int32)
    return pack(embed(quantize(v, power), power.astype(jnp.int32) + BIAS, count))


def decode(packed):
    code = unpack(packed)
    return code.astype(jnp.float32) * scale_of(code)


def group_of(half):
    return min(GROUP, half)


def publish_code(v):
    half = v.shape[0] // 2
    size = group_of(half)
    lane = lax.broadcasted_iota(jnp.int32, (size, LANES), 1)
    out = []
    for g in range(half // size):
        hi, lo = v[g * size : (g + 1) * size], v[half + g * size : half + (g + 1) * size]
        top = jnp.max(jnp.maximum(jnp.abs(hi), jnp.abs(lo)), axis=0, keepdims=True)
        top = jnp.maximum(jnp.max(top, axis=1, keepdims=True), TINY)
        word = jnp.ceil(jnp.log2(top) * FINE)
        factor = jnp.exp2(word * (-1.0 / FINE)) * STEPS
        codes = [jnp.floor(part * factor + 0.5).astype(jnp.int32) for part in (hi, lo)]
        bit = lax.shift_right_logical(
            jnp.broadcast_to(word.astype(jnp.int32) + FINE_BIAS, (size, LANES)), jnp.minimum(lane, 31)
        ) & 1
        first = (codes[0] & jnp.where(lane < FINE_BITS, -2, -1)) | jnp.where(lane < FINE_BITS, bit, 0)
        out.append((first << 16) | (codes[1] & 0xFFFF))
    return jnp.concatenate(out, axis=0)


TUNED = {
    (4, 4, 8): (
        0, 15, 17, 21, 31, 2, 13, 16, 26, 33, 32, 40, 34, 44, 55, 69, 92, 65, 100, 125,
        66, 78, 131, 81, 90, 142, 76, 93, 111, 88, 120, 127, 80, 96, 137, 1, 18, 22, 35, 37,
        3, 20, 23, 39, 41, 38, 49, 42, 54, 61, 71, 118, 72, 112, 135, 74, 102, 134, 83, 97,
        130, 79, 94, 117, 98, 106, 129, 95, 114, 144, 25, 46, 50, 57, 60, 30, 53, 56, 63, 67,
        64, 75, 68, 77, 86, 101, 136, 109, 132, 105, 126, 113, 139, 119, 143, 121, 145, 124, 146, 4,
        24, 29, 43, 45, 5, 28, 36, 48, 51, 47, 59, 52, 58, 73, 82, 104, 91, 115, 87, 128,
        103, 141, 108, 122, 107, 133, 116, 140, 6, 7, 12, 14, 19, 8, 9, 10, 11, 27, 62, 70,
        84, 85, 89, 99, 110, 123, 138,
    ),
}


def schedule(z_n, pairs, tiles):
    times = {}
    for p in range(pairs):
        at = 9.0 + 3.0 * p
        for s in range(2):
            times["P", p, s] = 0.01 * p if p < pairs - 1 else 9.1
            times["A", p, s] = at + 0.01 * s
            times["B1", p, s] = at + 0.1 + 0.01 * s
            times["B2", p, s] = at + 0.5 + 0.01 * s
            times["C", p, s] = at + 8.0 + 0.01 * s
        steps = (z_n - 1).bit_length()
        for s in range(2):
            times["Z", p, s] = at + 8.1 + 0.01 * s
            for b in range(1, steps):
                times["H", p, b, s] = at + 8.0 + 5.5 * b + 0.01 * s
        done = max(26.0 + 4.0 * p, at + 8.0 + 5.5 * steps)
        times["D", p] = done
        if p >= pairs - LATE:
            times["F", p] = done + 3.2
        for k in range(z_n):
            for d in range(2 if k else 1):
                if k:
                    times["E", p, k, d] = done + 3.5 * k
                if p < pairs - LATE:
                    times["R", p, k, d] = done + 3.5 * k + 3.2
                times["S", p, k, d] = done + 3.5 * k + 6.8
    times["mate",] = 0.005
    for s in range(2):
        times["hitO", s] = 2.0 + 0.1 * s
        times["hitN", s] = 4.6 + 0.1 * s
        times["own", s, 1] = 4.0 + 0.1 * s
        times["own", s, 0] = 4.3 + 0.1 * s
    for i in range(tiles):
        times["L", i] = 26.5 + 1.5 * i
    times["X",] = 27.0 + 1.5 * tiles
    times["Y",] = 33.0 + 1.5 * tiles
    tuned = TUNED.get((z_n, pairs, tiles))
    if tuned is not None:
        times = dict(zip(times, tuned, strict=True))
    return sorted(times, key=lambda task: times[task])


def update_kernel(
    z_n, pairs, p_hbm, c_hbm, assign_hbm, keep_hbm, code_hbm, cost_ref,
    out_ref, p2, cents, ak, prior, idv, slot, hit, pn, acc, cnt, asend, arecv, zsend, zrecv, low, lowr,
    loc, ids_s, ids_r, mt_s, mt_r, ps, pr, fs, fr, as_, ar, zs, zr,
    grs, grr, gls, glr, xs, xr, ys, yr, ds_, dr, outs, f1s, f1r, f2s, f2r, hrs, hrr, hls, hlr, lo_s, lo_r,
):
    z, q, m = lax.axis_index("z"), lax.axis_index("q"), lax.axis_index("mp")
    nx = q + 1 - 2 * lax.rem(q, 2)
    ny = lax.rem(q + 2, PLANE)
    other = 1 - m
    rows, width = p_hbm.shape
    shard_rows = c_hbm.shape[0]
    block = prior.shape[0]
    both = 2 * rows
    kept = z_n * block
    side_w = width // 2
    part = side_w // pairs
    last = z_n - 1
    bits = last.bit_length()
    up, down = lax.rem(z + 1, z_n), lax.rem(z + last, z_n)
    own = z * PLANE + q
    near, far = (nx, ny), (ny, nx)

    load_p = pltpu.make_async_copy(p_hbm, p2.at[pl.ds(0, rows)], loc.at[0])
    load_prior = pltpu.make_async_copy(
        c_hbm.at[pl.ds(pl.multiple_of(own * block, block), block)], prior, loc.at[1]
    )
    load_c = pltpu.make_async_copy(c_hbm, cents, loc.at[2])
    load_a = pltpu.make_async_copy(assign_hbm, ak.at[0], loc.at[3])
    load_k = pltpu.make_async_copy(keep_hbm, ak.at[1], loc.at[4])
    for copy in (load_a, load_k, load_p):
        copy.start()

    barrier = pltpu.get_barrier_semaphore()
    peers = [(z, q, other), (z, nx, m), (z, nx, other), (z, ny, m), (z, ny, other)]
    greet = peers + [(lax.rem(z + k, z_n), q, m) for k in range(1, z_n)]
    for peer in greet:
        pl.semaphore_signal(barrier, inc=1, device_id=peer, device_id_type=MESH)
    load_a.wait()
    load_k.wait()
    idv[0] = jnp.where(ak[1] > 0, ak[0], -1)
    load_c.start()
    load_prior.start()
    pl.semaphore_wait(barrier, len(greet))

    def pts_copy(s, p):
        cols = pl.ds(s * side_w + p * part, part)
        return remote(
            p2.at[pl.ds(0, rows), cols], pn.at[s, pl.ds(0, rows), pl.ds(p * part, part)], ps.at[s, p], pr.at[s, p],
            (z, near[s], m),
        )

    def fwd_copy(s, p):
        return remote(
            pn.at[s, pl.ds(0, rows), pl.ds(p * part, part)], pn.at[s, pl.ds(rows, rows), pl.ds(p * part, part)], fs.at[s, p], fr.at[s, p],
            (z, q, other),
        )

    def a_copy(s, p):
        return remote(asend.at[s, p], arecv.at[s, p], as_.at[s, p], ar.at[s, p], (z, far[s], m))

    def side_of(s):
        return slice(s * (block // 2), (s + 1) * (block // 2))

    def z_copy(p, b, s):
        n = z_n >> (b + 1)
        at = pl.ds(z_n - 2 * n, n)
        bit = lax.rem(lax.div(z, 1 << b), 2)
        to = z + (1 << b) * (1 - 2 * bit)
        return remote(
            zsend.at[p, at, side_of(s)], zrecv.at[p, at, side_of(s)], zs.at[p, b, s], zr.at[p, b, s], (to, q, m)
        )

    id_copies = [
        remote(idv.at[0], idv.at[k + 1], ids_s.at[k], ids_r.at[k], peer) for k, peer in enumerate(peers)
    ]
    mate_copy = remote(p2.at[pl.ds(0, rows)], p2.at[pl.ds(rows, rows)], mt_s, mt_r, (z, q, other))

    load_p.wait()
    for copy in id_copies:
        copy.start()

    def slots_of(s, a, b):
        ids = jnp.concatenate([idv[a], idv[b]], axis=1) - m * shard_rows
        inside = (ids >= 0) & (ids < shard_rows)
        ids = jnp.where(inside, ids, 0)
        owner = lax.rem(lax.div(ids, block), PLANE)
        at = lax.div(ids, block * PLANE) * block + lax.rem(ids, block)
        found = jnp.where(owner == q, at, jnp.where(owner == far[s], at + kept, -1))
        return jnp.where(inside, found, -1)

    def fill_hits(s, first):
        group = s if first else 2 + s
        slot[s] = slots_of(s, *((0, 1) if first else ((2, 3), (4, 5))[s]))

        def tile(t, carry):
            base = pl.multiple_of(t * LANES, LANES)
            row = lax.broadcasted_iota(jnp.int32, (LANES, both), 0) + base
            hit[group, pl.ds(base, LANES), :] = jnp.where(row == slot[s], 1.0, 0.0).astype(jnp.bfloat16)
            return carry

        lax.fori_loop(0, 2 * kept // LANES, tile, 0)

    ones = jnp.ones((both, LANES), jnp.bfloat16)

    def own_dot(s, half):
        at = pl.ds(half * kept, kept)
        acc[s, at, :] = jnp.dot(
            hit[s, at, :], p2[:, s * side_w : (s + 1) * side_w], preferred_element_type=jnp.float32
        )
        if s == 0:
            cnt[at, :] = jnp.dot(hit[s, at, :], ones, preferred_element_type=jnp.float32)

    def near_dot(s, p, half):
        at, cols = pl.ds(half * kept, kept), pl.ds(p * part, part)
        points = pn[s, :, p * part : (p + 1) * part]
        if s == 0 and p == 0:
            points = jnp.concatenate([points, ones], axis=1)
        more = jnp.dot(hit[2 + s, at, :], points, preferred_element_type=jnp.float32)
        acc[s, at, cols] += more[:, :part]
        if s == 0 and p == 0:
            cnt[at, :] += more[:, part:]

    def rows_of(t):
        return span(t, block)

    def half_rows_of(t):
        return span(t, block // 2)

    def step_a(p, s):
        pts_copy(s, p).wait_recv()
        fwd_copy(s, p).start()

    def step_b(p, s):
        fwd_copy(s, p).wait_recv()
        near_dot(s, p, 1)

        def tile(t):
            at = span(t, block, kept)
            count = cnt[at, 0:1] if s == 0 and p == 0 else None
            asend[s, p, half_rows_of(t), :] = encode(acc[s, at, p * part : (p + 1) * part], count)

        repeat(z_n, tile)
        a_copy(s, p).start()

    def step_b2(p, s):
        near_dot(s, p, 0)

    def target(b, j, mine):
        bit = lax.rem(lax.div(z, 1 << b), 2)
        return j * (2 << b) + lax.rem(z, 1 << b) + (bit if mine else 1 - bit) * (1 << b)

    def z_send(p, b, s):
        n = z_n >> (b + 1)

        def tile(j):
            at = rows_of(target(b, j, False))
            count = cnt[at, 0:1] if s == 0 and p == 0 else None
            zsend[p, z_n - 2 * n + j, side_of(s), :] = encode(acc[s, at, p * part : (p + 1) * part], count)

        repeat(n, tile)
        z_copy(p, b, s).start()

    def gain(s, p, at, packed):
        acc[s, at, p * part : (p + 1) * part] += decode(packed)
        if s == 0 and p == 0:
            cnt[at, :] = jnp.broadcast_to(cnt[at, 0:1] + count_of(unpack(packed)), (block, LANES))

    def step_c(p, s):
        a_copy(s, p).wait_recv()

        def tile(t):
            gain(s, p, rows_of(t), arecv[s, p, half_rows_of(t), :])

        repeat(z_n, tile)

    def z_gain(p, b, s):
        n = z_n >> (b + 1)
        z_copy(p, b, s).wait_recv()

        def tile(j):
            gain(s, p, rows_of(target(b, j, True)), zrecv[p, z_n - 2 * n + j, side_of(s), :])

        repeat(n, tile)

    def step_h(p, b, s):
        z_gain(p, b - 1, s)
        z_send(p, b, s)

    def xcopy(p, n, to_q):
        at = out_ref.at[p, n * PLANE + to_q]
        return remote(at, at, xs.at[p, n], xr.at[p, n], (z, nx, m))

    def ycopy(p, n, to_q):
        at = out_ref.at[p, n * PLANE + to_q]
        return remote(at, at, ys.at[p, n], yr.at[p, n], (z, ny, m))

    def dcopy(p, n, by_x):
        at = out_ref.at[p, n * PLANE + (nx if by_x else ny)]
        return remote(at, at, ds_.at[p, n], dr.at[p, n], (z, ny if by_x else nx, m))

    def gright(p, n):
        at = out_ref.at[p, n * PLANE + q]
        return remote(at, at, grs.at[p, n], grr.at[p, n], (up, q, m))

    def gleft(p, n):
        at = out_ref.at[p, n * PLANE + q]
        return remote(at, at, gls.at[p, n], glr.at[p, n], (down, q, m))

    def late(p):
        return p >= pairs - LATE

    def first_copy(p, s):
        at = out_ref.at[p, own, side_of(s)]
        return remote(at, at, f1s.at[p, s], f1r.at[p, s], (z, near[s], m))

    def second_copy(p, n, s, j):
        at = out_ref.at[p, n * PLANE + (near[s] if j else q), side_of(s)]
        i = 2 * s + j
        return remote(at, at, f2s.at[p, n, i], f2r.at[p, n, i], (z, far[s], m))

    def hright(p, n, s):
        at = out_ref.at[p, n * PLANE + near[s], side_of(s)]
        return remote(at, at, hrs.at[p, n, s], hrr.at[p, n, s], (up, q, m))

    def hleft(p, n, s):
        at = out_ref.at[p, n * PLANE + near[s], side_of(s)]
        return remote(at, at, hls.at[p, n, s], hlr.at[p, n, s], (down, q, m))

    def step_f(p):
        for s in range(2):
            first_copy(p, s).wait_recv()

        @pl.when(z < last)
        def _():
            for s in range(2):
                hright(p, z, s).start()

        @pl.when(z > 0)
        def _():
            for s in range(2):
                hleft(p, z, s).start()

        for s in range(2):
            second_copy(p, z, s, 1).start()

    def step_d(p):
        mine = rows_of(z)
        for s in range(2):
            z_gain(p, bits - 1, s)
        if p == 0:
            load_prior.wait()
        count = cnt[mine, 0:1]
        fresh = []
        for s in range(2):
            lo = s * side_w + p * part
            total = acc[s, mine, p * part : (p + 1) * part]
            fallback = prior[:, lo : lo + part].astype(jnp.float32)
            fresh.append(jnp.where(count > 0.5, total / jnp.maximum(count, 1.0), fallback))
        for s in range(2):
            out_ref[p, own, side_of(s)] = publish_code(fresh[s])

        @pl.when(z < last)
        def _():
            gright(p, z).start()

        @pl.when(z > 0)
        def _():
            gleft(p, z).start()

        if late(p):
            for s in range(2):
                first_copy(p, s).start()
            for s in range(2):
                second_copy(p, z, s, 0).start()
            return

        xcopy(p, z, q).start()
        ycopy(p, z, q).start()

    def relay(p, n, by_x):
        if by_x:
            xcopy(p, n, nx).wait_recv()
        else:
            ycopy(p, n, ny).wait_recv()
        dcopy(p, n, by_x).start()

    def settle(p, n, by_x):
        if late(p):
            for s in range(2):
                for j in range(2):
                    second_copy(p, n, s, j).wait_recv()
            put(p, n).start()
            return
        if by_x:
            ycopy(p, n, ny).wait_recv()
        else:
            xcopy(p, n, nx).wait_recv()
        dcopy(p, n, by_x).wait_recv()

        put(p, n).start()

    def put(p, n):
        at = pl.ds(n * PLANE, PLANE)
        return pltpu.make_async_copy(out_ref.at[p, at], code_hbm.at[p, at], outs.at[p, n])

    def each(p, k, d, action):
        if k == 0:
            action(p, z, p % 2 == 0)
            return

        @pl.when((z >= k) if d == 0 else (z + k <= last))
        def _():
            action(p, z - k if d == 0 else z + k, (k + p) % 2 == d)

    def spread(p, k, d):
        @pl.when((z >= k) if d == 0 else (z + k <= last))
        def _():
            n, hop = (z - k, gright) if d == 0 else (z + k, gleft)
            hop(p, n).wait_recv()

            @pl.when((z < last) if d == 0 else (z > 0))
            def _():
                hop(p, n).start()

            if not late(p):
                xcopy(p, n, q).start()
                ycopy(p, n, q).start()
                return

            for s in range(2):
                second_copy(p, n, s, 0).start()
            hops = hright if d == 0 else hleft
            for s in range(2):
                hops(p, n, s).wait_recv()

            @pl.when((z < last) if d == 0 else (z > 0))
            def _():
                for s in range(2):
                    hops(p, n, s).start()

            for s in range(2):
                second_copy(p, n, s, 1).start()

    met = []

    def meet():
        if not met:
            met.append(True)
            mate_copy.wait_recv()

    seen = []

    def lowest():
        i = len(seen)
        seen.append(i)
        meet()
        if i == 0:
            load_c.wait()

        def tile(t, best):
            tile_ref = cents[pl.ds(pl.multiple_of(t * CTILE, CTILE), CTILE), :]
            wide = tile_ref.astype(jnp.float32)
            sq = jnp.sum(wide * wide, axis=1, keepdims=True)
            inner = lax.dot_general(
                tile_ref, p2[...], (((1,), (1,)), ((), ())), preferred_element_type=jnp.float32
            )
            return jnp.minimum(best, jnp.min(sq - 2.0 * inner, axis=0, keepdims=True))

        start = jnp.full((1, both), jnp.inf, jnp.float32) if i == 0 else low[...]
        low[...] = lax.fori_loop(i, i + 1, tile, start)

    low_copy = remote(low.at[:, pl.ds(rows, rows)], lowr, lo_s, lo_r, (z, q, other))

    def finish_cost():
        low_copy.wait_recv()
        wide = p2[pl.ds(0, rows), :].astype(jnp.float32)
        sq = jnp.sum(wide * wide, axis=1, keepdims=True)
        flat = jnp.broadcast_to(sq, (rows, LANES)).T[0:1, :]
        cost_ref[...] = (flat + jnp.minimum(low[:, :rows], lowr[...])) / width

    greeted = []

    def hits(s, first):
        if not greeted:
            greeted.append(True)
            for copy in id_copies:
                copy.wait_recv()
        fill_hits(s, first)

    def own_part(s, half):
        meet()
        own_dot(s, half)

    actions = {
        "P": lambda p, s: pts_copy(s, p).start(), "mate": mate_copy.start,
        "hitO": lambda s: hits(s, True), "hitN": lambda s: hits(s, False), "own": own_part,
        "A": step_a, "B1": step_b, "B2": step_b2, "C": step_c, "Z": lambda p, s: z_send(p, 0, s), "H": step_h,
        "D": step_d, "F": step_f, "E": spread, "R": lambda p, k, d: each(p, k, d, relay),
        "S": lambda p, k, d: each(p, k, d, settle), "L": lambda i: lowest(),
        "X": low_copy.start, "Y": finish_cost,
    }
    for task in schedule(z_n, pairs, shard_rows // CTILE):
        actions[task[0]](*task[1:])

    for copy in id_copies + [mate_copy, low_copy]:
        copy.wait_send()
    for p in range(pairs):
        for s in range(2):
            if late(p):
                first_copy(p, s).wait_send()
            pts_copy(s, p).wait_send()
            fwd_copy(s, p).wait_send()
            a_copy(s, p).wait_send()
        for t in range(z_n):
            if t < bits:
                for s in range(2):
                    z_copy(p, t, s).wait_send()

            @pl.when((z >= t) & (z < last))
            def _(p=p, t=t):
                gright(p, t).wait_send()
                if late(p):
                    for s in range(2):
                        hright(p, t, s).wait_send()

            @pl.when((z <= t) & (z > 0))
            def _(p=p, t=t):
                gleft(p, t).wait_send()
                if late(p):
                    for s in range(2):
                        hleft(p, t, s).wait_send()

            put(p, t).wait()
            if late(p):
                for s in range(2):
                    for j in range(2):
                        second_copy(p, t, s, j).wait_send()
                continue
            xcopy(p, t, q).wait_send()
            ycopy(p, t, q).wait_send()
            dcopy(p, t, True).wait_send()


def decode_kernel(in_hbm, cost_in, out_hbm, cost_out, codes, fresh, cost, ins, outs, row):
    pairs, dp_n, block, part = codes.shape
    half = block // 2
    size = group_of(half)
    side_w = fresh.shape[1] // 2
    lane = lax.broadcasted_iota(jnp.int32, (1, LANES), 1)
    weight = jnp.where(lane < FINE_BITS, 1 << jnp.minimum(lane, FINE_BITS), 0).astype(jnp.float32)
    owners = max(1, min(dp_n, LANES // block))

    def load(i):
        at = pl.ds(i * owners, owners)
        return pltpu.make_async_copy(in_hbm.at[:, at], codes.at[:, at], ins.at[i])

    def store(i):
        at = pl.ds(i * owners * block, owners * block)
        return pltpu.make_async_copy(fresh.at[at], out_hbm.at[at], outs.at[i])

    for i in range(dp_n // owners):
        load(i).start()
    take = pltpu.make_async_copy(cost_in, cost, row.at[0])
    give = pltpu.make_async_copy(cost, cost_out, row.at[1])
    take.start()

    def owner(o, carry):
        for p in range(pairs):
            for s in range(2):
                cols = slice(s * side_w + p * part, s * side_w + (p + 1) * part)
                for g in range(half // size):
                    packed = codes[p, o, s * half + g * size : s * half + (g + 1) * size]
                    bits = ((packed[:8] >> 16) & 1).astype(jnp.float32)
                    word = jnp.sum(bits * weight, axis=1, keepdims=True) - FINE_BIAS
                    scale = jnp.exp2(word * (1.0 / FINE)) * (1.0 / STEPS)
                    scale = jnp.broadcast_to(scale[0:1], (1, part))
                    at = pl.multiple_of(o * block, block) + g * size
                    fresh[pl.ds(at, size), cols] = (packed >> 16).astype(jnp.float32) * scale
                    low = ((packed << 16) >> 16).astype(jnp.float32)
                    fresh[pl.ds(at + half, size), cols] = low * scale
        return carry

    for i in range(dp_n // owners):
        load(i).wait()
        lax.fori_loop(i * owners, (i + 1) * owners, owner, 0)
        store(i).start()
    take.wait()
    give.start()
    for i in range(dp_n // owners):
        store(i).wait()
    give.wait()


def shards(points, centroids, assign, keep_mask):
    rows, width = points.shape
    shard_rows = centroids.shape[0]
    z_n = lax.axis_size("z")
    dp_n = z_n * PLANE
    block = shard_rows // dp_n
    kept = z_n * block
    part = LANES
    side_w = width // 2
    pairs = side_w // part
    vmem = pl.BlockSpec(memory_space=pltpu.VMEM)
    hbm = pl.BlockSpec(memory_space=pltpu.HBM)
    dma = pltpu.SemaphoreType.DMA
    by_pair = dma((2, pairs))
    by_z = dma((pairs, z_n))
    halves = dma((pairs, 2))
    by_step = dma((pairs, (z_n - 1).bit_length(), 2))
    by_half = dma((pairs, z_n, 2))
    by_quarter = dma((pairs, z_n, 4))
    codes, cost = pl.pallas_call(
        functools.partial(update_kernel, z_n, pairs),
        out_shape=(
            jax.ShapeDtypeStruct((pairs, dp_n, block, part), jnp.int32),
            jax.ShapeDtypeStruct((1, rows), jnp.float32),
        ),
        in_specs=[hbm] * 4,
        out_specs=(hbm, vmem),
        scratch_shapes=[
            pltpu.VMEM((pairs, dp_n, block, part), jnp.int32),
            pltpu.VMEM((2 * rows, width), points.dtype),
            pltpu.VMEM((shard_rows, width), centroids.dtype),
            pltpu.VMEM((2, 1, rows), jnp.int32),
            pltpu.VMEM((block, width), centroids.dtype),
            pltpu.VMEM((6, 1, rows), jnp.int32),
            pltpu.VMEM((2, 1, 2 * rows), jnp.int32),
            pltpu.VMEM((4, 2 * kept, 2 * rows), jnp.bfloat16),
            pltpu.VMEM((2, 2 * rows, side_w), points.dtype),
            pltpu.VMEM((2, 2 * kept, side_w), jnp.float32),
            pltpu.VMEM((2 * kept, LANES), jnp.float32),
            pltpu.VMEM((2, pairs, kept // 2, part), jnp.int32),
            pltpu.VMEM((2, pairs, kept // 2, part), jnp.int32),
            pltpu.VMEM((pairs, z_n, block, part), jnp.int32),
            pltpu.VMEM((pairs, z_n, block, part), jnp.int32),
            pltpu.VMEM((1, 2 * rows), jnp.float32),
            pltpu.VMEM((1, rows), jnp.float32),
            dma((5,)), dma((5,)), dma((5,)), dma, dma,
            by_pair, by_pair, by_pair, by_pair, by_pair, by_pair,
            by_step, by_step, by_z, by_z, by_z, by_z, by_z, by_z, by_z, by_z, by_z, by_z, by_z,
            halves, halves, by_quarter, by_quarter, by_half, by_half, by_half, by_half,
            dma, dma,
        ],
        compiler_params=pltpu.CompilerParams(
            collective_id=0, has_side_effects=True, vmem_limit_bytes=56 * 1024 * 1024
        ),
        cost_estimate=pl.CostEstimate(
            flops=0, bytes_accessed=200 * 1024 * 1024, transcendentals=0
        ),
        name="update",
    )(points, centroids, assign.reshape(1, rows), keep_mask.reshape(1, rows))
    new_centroids, cost = pl.pallas_call(
        decode_kernel,
        in_specs=[hbm, hbm],
        out_specs=(hbm, hbm),
        out_shape=(
            jax.ShapeDtypeStruct((shard_rows, width), jnp.float32),
            jax.ShapeDtypeStruct((1, rows), jnp.float32),
        ),
        scratch_shapes=[
            pltpu.VMEM((pairs, dp_n, block, part), jnp.int32),
            pltpu.VMEM((shard_rows, width), jnp.float32),
            pltpu.VMEM((1, rows), jnp.float32),
            dma((dp_n,)), dma((dp_n,)), dma((2,)),
        ],
        compiler_params=pltpu.CompilerParams(vmem_limit_bytes=56 * 1024 * 1024),
        name="decode",
    )(codes, cost)
    return new_centroids, cost.reshape(rows)


def solution(mesh):
    dp, mp = mesh.shape["dp"], mesh.shape["mp"]
    grid = Mesh(mesh.devices.reshape(dp // PLANE, PLANE, mp), ("z", "q", "mp"))
    rows = ("z", "q", "mp")
    in_specs = (P(rows, None), P("mp", None), P(rows), P(rows))
    out_specs = (P("mp", None), P(rows))
    return jax.shard_map(shards, mesh=grid, in_specs=in_specs, out_specs=out_specs, check_vma=False)
```
